32 devices in a mesh: seq: 4 (over z), exp: 8 (over y, x, core).
Axes of the slice: x: 2, y: 2, z: 4, core: 2. Of those that a mesh axis runs over, the one named last changes fastest.
Arguments:
- tokens: bfloat16 [20480, 4096], P(('seq', 'exp')), may hold values from -6 to 6
- routes: int32 [20480, 2], P(('seq', 'exp')), may hold values from 0 to 15, all different within a row; in each aligned block of 640 rows (0 to 639, 640 to 1279, ...) at most 100 rows name the same one
- gates: float32 [20480, 2], P(('seq', 'exp')), may hold values from 0.1 to 1
- weights: bfloat16 [16, 4096, 1024], P('exp', 'seq'), may hold values from -0.09375 to 0.09375
Outputs:
- mixed: bfloat16 [20480, 1024], P(('seq', 'exp'))
The draws below stay inside these ranges and needn't reach their ends.
Inputs may be any that keep to these rules, and one draw needn't show every extreme that they name: `routes`: the two experts of a token differ. Among the rows of one device no expert is named more than 100 times, a bound that some block reaches.
All inputs are finite; a program needn't handle non-finite values.
Results may differ from the reference program's by a relative error of at most 0.0049.
Values may be sent and summed in bfloat16 or wider, within the bound.
A program may use at most 192 MiB of HBM per device.

```python
import math
import jax
import jax.numpy as jnp
import numpy as np
from jax import lax

D = 4096
FF = 1024
TOK_DEV = 640
EXPERTS = 16
CAP = 100
TOKENS = 20480


def levels(rng, shape, shards, low, high):
    factor_of = 1.0
    for dim, shards_of in shards:
        draws = jax.random.uniform(jax.random.fold_in(jax.random.fold_in(rng, 6), dim), (shards_of,), jnp.float32, low / len(shards), high / len(shards))
        factor_of = factor_of * jnp.repeat(jnp.exp(draws), shape[dim] // shards_of).reshape((-1,) + (1,) * (len(shape) - 1 - dim))
    return factor_of


def deal_out(stream_key, own, number, rows, amount, top, limit, slope):
    sequence = jax.random.permutation(stream_key, amount)
    crowded, common = shares(amount, rows * top, limit, slope, True), shares(amount, rows * top, limit, slope, False)
    places = jnp.arange(amount)

    def named(lengths, turn):
        used = int((lengths > 0).sum())
        fixed = max(1, used // 4)
        shifted = fixed + (places - fixed + turn * (used - fixed)) % max(1, amount - fixed)
        return jnp.zeros((amount,), jnp.int32).at[sequence[jnp.where(places < fixed, places, shifted)]].set(jnp.asarray(lengths, jnp.int32))

    lengths = jnp.where(number % 4 == 0, named(crowded, number // 4), named(common, number - number // 4 - 1))
    mixed = jax.random.permutation(jax.random.fold_in(own, 3), amount)
    donor, sink = mixed[0:amount // 2 * 2:2], mixed[1:amount // 2 * 2:2]
    margin = jnp.minimum(lengths[donor] - 1, limit - lengths[sink]) // 2
    margin = jnp.where((donor == sequence[0]) | (sink == sequence[0]) | (lengths[sink] == 0), 0, jnp.maximum(margin, 0))
    shifted = jax.random.randint(jax.random.fold_in(own, 4), (amount // 2,), 0, 1 << 20) % (margin + 1)
    lengths = lengths.at[donor].add(-shifted).at[sink].add(shifted)
    items = jnp.searchsorted(jnp.cumsum(lengths), jnp.arange(rows * top), side="right").astype(jnp.int32)
    grid = items.reshape(top, rows).T
    grid = grid[jax.random.permutation(jax.random.fold_in(own, 1), rows)]
    turn = jax.random.randint(jax.random.fold_in(own, 2), (rows, 1), 0, top)
    return jnp.take_along_axis(grid, (jnp.arange(top)[None, :] + turn) % top, axis=1)


def shares(number_of, total, most, skew, full):
    weights = [(1 << 20) // math.isqrt(standing ** skew) + 1 for standing in range(1, number_of + 1)]
    largest = most if full else min(most, max(-(-total // number_of), total * weights[0] // sum(weights)))
    least = 1 if total - largest >= number_of - 1 else 0
    holding, rest = [largest] + [least] * (number_of - 1), total - largest - least * (number_of - 1)
    while rest > 0:
        free = [i for i in range(1, number_of) if holding[i] < largest] or [i for i in range(1, number_of) if holding[i] < most]
        mass, budget = sum([weights[i] for i in free]), rest
        for i in free:
            more = min(most - holding[i], max(1, budget * weights[i] // mass), rest)
            holding[i] = holding[i] + more
            rest = rest - more
    return np.array(holding)


def scatter_about(rng, extent, scale, most, pieces=(), held_as=jnp.bfloat16):
    gain = levels(rng, extent, pieces, -0.22, 0.18) if pieces else 1.0
    drawn = jax.random.normal(rng, extent, jnp.float32) * scale * gain
    return jnp.minimum(jnp.maximum(drawn, -most), most).astype(held_as)


def setup_inputs(seed: int = 0) -> dict:
    seeds = jax.random.split(jax.random.key(seed), 5)
    tokens = scatter_about(seeds[0], (TOKENS, D), 1.0, 6.0, ((0, 32),))
    routes_keys = jax.random.split(jax.random.fold_in(seeds[1], 1), TOKENS // TOK_DEV)
    routes_turns = jax.random.permutation(jax.random.fold_in(seeds[1], 3), TOKENS // TOK_DEV)
    routes = jax.vmap(lambda own, number: deal_out(jax.random.fold_in(seeds[1], 2), own, number, TOK_DEV, EXPERTS, 2, CAP, 2))(routes_keys, routes_turns).reshape((TOKENS, 2))
    gates = jnp.clip(0.1 + 0.9 * jax.random.uniform(seeds[2], (TOKENS, 2), jnp.float32) ** levels(seeds[2], (TOKENS, 2), ((0, 32),), -0.2, 0.2), 0.1, 1.0)
    weights = scatter_about(seeds[3], (EXPERTS, D, FF), D ** -0.5, 0.09375, ((0, 8), (1, 4)))
    return dict(tokens=tokens, routes=routes, gates=gates, weights=weights)


def route_slots(route_block, experts, capacity):
    expert_ids = route_block.reshape(-1)
    one_hot = (expert_ids[:, None] == jnp.arange(experts, dtype=jnp.int32)[None, :]).astype(jnp.int32)
    earlier = jnp.cumsum(one_hot, axis=0) - one_hot
    slot_index = jnp.sum(earlier * one_hot, axis=1)
    return (expert_ids * capacity + slot_index).astype(jnp.int32)


def reference(tokens, routes, gates, weights):
    blocks = TOKENS // TOK_DEV
    route_blocks = routes.reshape(blocks, TOK_DEV, 2)
    position = jax.vmap(lambda block: route_slots(block, EXPERTS, CAP))(route_blocks)
    local_rows = jnp.arange(2 * TOK_DEV, dtype=jnp.int32) // 2
    block_base = (jnp.arange(blocks, dtype=jnp.int32) * TOK_DEV)[:, None]
    global_rows = block_base + local_rows[None, :]

    def fill_table(places, rows):
        return jnp.full((EXPERTS * CAP,), TOKENS, jnp.int32).at[places].set(rows)

    slot_rows = jax.vmap(fill_table)(position, global_rows).reshape(blocks, EXPERTS, CAP)
    padded = jnp.concatenate([tokens, jnp.zeros((1, D), jnp.bfloat16)], axis=0)

    def one_expert(expert):
        indices = lax.dynamic_index_in_dim(slot_rows, expert, 1, keepdims=False).reshape(-1)
        gathered = padded[indices]
        matrix = lax.dynamic_index_in_dim(weights, expert, 0, keepdims=False)
        return jnp.dot(gathered, matrix, preferred_element_type=jnp.float32).astype(jnp.bfloat16)

    outputs = lax.map(one_expert, jnp.arange(EXPERTS, dtype=jnp.int32))
    outputs = outputs.reshape(EXPERTS * blocks * CAP, FF)
    expert_ids = route_blocks.reshape(blocks, 2 * TOK_DEV)
    slot_index = position - expert_ids * CAP
    block_ids = jnp.arange(blocks, dtype=jnp.int32)[:, None]
    flat_index = ((expert_ids * blocks + block_ids) * CAP + slot_index).reshape(-1)
    picked = outputs[flat_index].reshape(TOKENS, 2, FF).astype(jnp.float32)
    mixed = jnp.sum(picked * gates[:, :, None], axis=1)
    return mixed.astype(jnp.bfloat16)
```

```python
import functools

import jax
import jax.numpy as jnp
from jax import lax
from jax.experimental import pallas as pl
from jax.experimental.pallas import tpu as pltpu
from jax.sharding import PartitionSpec as P

COLUMN_PARTS = (1, 1)


def project_kernel(per_step, x_ref, gate_ref, w_ref, *rest):
    out_ref = rest[-1]
    step = pl.program_id(0)
    lanes = lax.broadcasted_iota(jnp.int32, gate_ref.shape, 1)

    @pl.when(step == 0)
    def _():
        out_ref[...] = jnp.zeros_like(out_ref)

    total = out_ref[...]
    for own in range(per_step):
        expert = step * per_step + own
        gate = jnp.sum(jnp.where(lanes == expert, gate_ref[...], 0.0), axis=1, keepdims=True)
        total += gate * jnp.dot(x_ref[...], w_ref[own], preferred_element_type=jnp.float32)
    out_ref[...] = total


def project(x, gate, weights, before):
    rows, depth = x.shape
    experts, _, cols = weights.shape
    per_step = 2
    return pl.pallas_call(
        functools.partial(project_kernel, per_step),
        grid=(experts // per_step,),
        out_shape=jax.ShapeDtypeStruct((rows, cols), jnp.float32),
        in_specs=[
            pl.BlockSpec((rows, depth), lambda e: (0, 0)),
            pl.BlockSpec((rows, experts), lambda e: (0, 0)),
            pl.BlockSpec((per_step, depth, cols), lambda e: (e, 0, 0)),
        ]
        + [pl.BlockSpec(memory_space=pl.ANY)] * len(before),
        out_specs=pl.BlockSpec((rows, cols), lambda e: (0, 0)),
        compiler_params=pltpu.CompilerParams(vmem_limit_bytes=32 * 1024 * 1024),
        cost_estimate=pl.CostEstimate(
            flops=2 * rows * depth * cols * experts,
            bytes_accessed=2 * experts * depth * cols + 2 * rows * depth,
            transcendentals=0,
        ),
    )(x, gate, weights, *before)


def shift_order(planes):
    near = [d for pair in zip(range(1, planes), range(planes - 1, 0, -1)) for d in pair]
    return list(dict.fromkeys(near))


def unit_order(planes, parts):
    early = 1
    arrival = [0] + shift_order(planes)
    order = [(d, q) for q in range(early) for d in arrival[:-1]]
    order += [(arrival[-1], q) for q in range(early)]
    for q in range(early, parts):
        order += [(d, q) for d in list(range(1, planes)) + [0]]
    return order


def spread_body(tokens, routes, gates, weights):
    experts = weights.shape[0] * lax.axis_size("exp")
    planes = lax.axis_size("seq")
    plane = lax.axis_index("seq")
    depth = weights.shape[1]
    share = weights.shape[2] // sum(COLUMN_PARTS)
    edges = [share * sum(COLUMN_PARTS[:q]) for q in range(len(COLUMN_PARTS) + 1)]

    def moved(value, shift):
        return lax.ppermute(value, "seq", [(i, (i + shift) % planes) for i in range(planes)])

    def features(target):
        return lax.dynamic_slice_in_dim(tokens, target * depth, depth, 1)

    dense = jnp.sum(
        jnp.where(
            routes[:, None, :] == jnp.arange(experts, dtype=jnp.int32)[None, :, None],
            gates[:, None, :],
            0.0,
        ),
        axis=2,
    )
    sent = dense.T
    gate, x = {0: dense}, {0: features(plane)}
    for shift in range(1, planes):
        gate[shift] = moved(sent, shift).T
    latest = None
    for shift in shift_order(planes):
        piece = features(lax.rem(plane + shift, planes))
        if latest is not None:
            piece, _ = lax.optimization_barrier((piece, latest))
        latest = x[shift] = moved(piece, shift)
    whole = [
        lax.all_gather(weights[:, :, edges[q] : edges[q + 1]], "exp", axis=0, tiled=True)
        for q in range(len(COLUMN_PARTS))
    ]
    parts, running, flying, stage, started = {}, {}, {}, {}, {}
    previous = []
    for index, (shift, q) in enumerate(unit_order(planes, len(COLUMN_PARTS))):
        landed = [key for key in flying if started[key] <= index - 2 and index >= planes]
        done = project(x[shift], gate[shift], whole[q], previous + [flying.pop(key) for key in landed])
        previous = [done]
        parts[shift, q] = done
        at = stage.get(q, 1)
        while at <= planes and (at % planes, q) in parts:
            begin = index
            value = parts[at % planes, q]
            if at > 1:
                value = running[q].astype(jnp.float32) + value
                begin = max(begin, started[at - 1, q] + 1)
            running[q] = value.astype(jnp.bfloat16)
            if at < planes:
                running[q] = moved(running[q], 1)
                flying[at, q] = running[q]
                started[at, q] = begin
            at += 1
        stage[q] = at
    return jnp.concatenate([running[q] for q in range(len(COLUMN_PARTS))], axis=1)


MESH = pl.DeviceIdType.MESH
PARTS = 4
BATCH = 4


def tree(size, local):
    digits = size.bit_length() - 1
    high = list(range(1, digits))

    def order(own):
        turn = own % max(1, len(high))
        return high[turn:] + high[:turn] + [0]

    def last(delta, own):
        return max((order(own).index(b) for b in range(digits) if delta >> b & 1), default=-1)

    def children(delta, own):
        return [b for b in order(own)[last(delta, own) + 1 :]]

    groups = [[(0, own) for own in range(local)]]
    for turn in range(local):
        groups.append([(1 << b, sorted(range(local), key=lambda own: order(own).index(b))[turn]) for b in high])
    for hops in range(2, digits):
        far = [h << 1 for h in range(size // 2) if bin(h).count("1") == hops]
        groups.append([(h, own) for h in far for own in range(local)])
    return groups, children


def line_order(planes):
    middle = (planes - 1) / 2
    return [sorted(range(planes), key=lambda d: (abs(d - p), abs(d - middle), d)) for p in range(planes)]


def schedule(planes, parts, groups):
    step, hop, slot = 1.7, 10.0, 12.0
    landed = [0.0, 32.0, 92.0, 120.0] + [120.0] * planes
    late = [(o, q) for o in range(2, planes) for q in range(parts - 1)]
    items, places, begun = [], {}, {}
    for q in range(parts):
        for g in range(groups):
            now = slot * (q * groups + g)
            first = [(0, q, g)]
            work = []
            if q == 0:
                if g == groups - 1:
                    work = [(1, 0, i) for i in range(groups)] if planes > 1 else []
                work = first + work
            else:
                work = first + ([(1, q, g)] if planes > 1 else [])
            if (q, g) >= (parts - 2, groups - 2) and late:
                work = [(*late[0], i) for i in range(groups)] + work
                late = late[1:]
            if (q, g) == (parts - 1, groups - 1):
                rest = [(o, k, i) for o, k in late for i in range(groups)]
                rest += [(o, q, i) for o in range(planes - 1, 1, -1) for i in range(groups)]
                work = rest + work[::-1]
            places[q, g] = (len(items), now)
            items += work
    clock, start, ended = 0.0, [], {}
    at = {index: now for index, now in places.values()}
    for index, (o, q, g) in enumerate(items):
        clock = max(clock, at.get(index, 0.0), landed[o])
        start.append(clock)
        begun.setdefault(o, index)
        clock += step
        ended[o, q] = clock
    order = line_order(planes)
    ready = {}
    for q in range(parts):
        for d in range(planes):
            for p in list(range(d)) + list(range(planes - 1, d, -1)) + [d]:
                time = ended[order[p].index(d), q]
                before = [p - 1] if p < d else [p + 1] if p > d else [p - 1, p + 1]
                for other in before:
                    if 0 <= other < planes:
                        time = max(time, ready[other, d, q] + hop)
                ready[p, d, q] = time
    sums = {}
    for p in range(planes):
        end = len(items)
        for time, d, q in sorted((ready[p, d, q], d, q) for d in range(planes) for q in range(parts)):
            where = next((i for i, begin in enumerate(start) if begin >= time), None)
            if where is None:
                where, end = end, end + 1
            sums.setdefault(where, {}).setdefault(p, []).append((d, q))
    return items, {index: key for key, (index, _) in places.items()}, begun, sums


def pick(which, values, default=0):
    found = jnp.int32(default)
    for index, value in enumerate(values):
        found = jnp.where(which == index, jnp.int32(value), found)
    return found


def fused_kernel(planes, size, tokens, weights, gate_in, out, w_buf, x_buf, t_buf, g_buf, acc, s_buf, o_buf, *sems):
    w_load, w_send, w_recv, x_load, x_send, x_recv, t_send, t_recv, s_send, s_recv, o_sem = sems
    plane, me = lax.axis_index("seq"), lax.axis_index("exp")
    local = weights.shape[0]
    rows, depth = x_buf.shape[1:]
    cols = o_buf.shape[2]
    parts = o_buf.shape[0]
    batches = w_buf.shape[0] // BATCH
    groups, children = tree(size, local)
    arrival = [chunk for group in groups for chunk in group + [(delta | 1, own) for delta, own in group]]
    place = {chunk: index for index, chunk in enumerate(arrival)}
    digits = size.bit_length() - 1
    items, events, begun, sums = schedule(planes, parts, len(groups))
    orders = line_order(planes)
    planes_of = [pick(plane, [orders[p][o] for p in range(planes)]) for o in range(planes)]
    near = [me + (1 - 2 * (lax.div(me, jnp.int32(1 << b)) % 2)) * (1 << b) for b in range(digits)]

    barrier = pltpu.get_barrier_semaphore()
    own_loads = [
        pltpu.make_async_copy(
            weights.at[own, :, pl.ds(q * cols, cols)], w_buf.at[place[0, own], q], w_load.at[own, q]
        )
        for q in range(parts)
        for own in range(local)
    ]
    own_rows = pltpu.make_async_copy(
        tokens.at[:, pl.ds(pl.multiple_of(plane * depth, depth), depth)], x_buf.at[plane], x_load
    )
    for load in own_loads[:local]:
        load.start()
    own_rows.start()
    for load in own_loads[local:]:
        load.start()
    for b in range(digits):
        pl.semaphore_signal(barrier, inc=1, device_id={"exp": near[b]}, device_id_type=MESH)
    for shift in range(1, planes):
        pl.semaphore_signal(
            barrier, inc=1, device_id={"seq": lax.rem(plane + shift, planes)}, device_id_type=MESH
        )
    pl.semaphore_wait(barrier, digits + planes - 1)

    def rows_to(target):
        return pltpu.make_async_remote_copy(
            src_ref=tokens.at[:, pl.ds(pl.multiple_of(target * depth, depth), depth)],
            dst_ref=x_buf.at[plane],
            send_sem=x_send.at[target],
            recv_sem=x_recv.at[plane],
            device_id={"seq": target},
            device_id_type=MESH,
        )

    def gates_to(target):
        return pltpu.make_async_remote_copy(
            src_ref=gate_in,
            dst_ref=t_buf.at[plane],
            send_sem=t_send.at[target],
            recv_sem=t_recv.at[plane],
            device_id={"seq": target},
            device_id_type=MESH,
        )

    for distance in range(1, planes):
        for target in (plane + distance, plane - distance):

            @pl.when((target >= 0) & (target < planes))
            def _():
                gates_to(target).start()
                rows_to(target).start()

    sent = []

    def pass_on(delta, own, b, q):
        copy = pltpu.make_async_remote_copy(
            src_ref=w_buf.at[place[delta, own], q],
            dst_ref=w_buf.at[place[delta ^ (1 << b), own], q],
            send_sem=w_send.at[q, count(delta, own, b)],
            recv_sem=w_recv.at[place[delta ^ (1 << b), own], q],
            device_id={"exp": near[b]},
            device_id_type=MESH,
        )
        return copy

    edges = [(delta, own, b) for group in groups for delta, own in group for b in children(delta, own)]

    def count(*edge):
        return edges.index(edge)

    def send_own(q):
        for own in range(local):
            own_loads[q * local + own].wait()
        for group in groups[1 : local + 1]:
            for delta, own in group:
                pass_on(0, own, delta.bit_length() - 1, q).start()
        for own in range(local):
            pass_on(0, own, 0, q).start()

    def landing(chunk, q):
        index = place[chunk]
        return pltpu.make_async_copy(w_buf.at[index, q], w_buf.at[index, q], w_recv.at[index, q])

    def arrive(q, g):
        if g == 0 and q == 0:
            send_own(0)
        if g > 0:
            for delta, own in groups[g]:
                landing((delta, own), q).wait()
                for b in children(delta, own):
                    pass_on(delta, own, b, q).start()
        if g == len(groups) - 2 and q + 1 < parts:
            send_own(q + 1)
        for delta, own in groups[g]:
            landing((delta | 1, own), q).wait()

    def meet(o):
        d = planes_of[o]
        if o == 0:
            own_rows.wait()
            g_buf[d] = gate_in[...].T
        else:
            pltpu.make_async_copy(x_buf.at[d], x_buf.at[d], x_recv.at[d]).wait()
            pltpu.make_async_copy(t_buf.at[d], t_buf.at[d], t_recv.at[d]).wait()
            g_buf[d] = t_buf[d].T

    block = 64 if rows % 64 == 0 else rows

    def sum_out(d, o, q):
        right = d > plane
        onward = jnp.where(right, plane + 1, plane - 1)
        slot = jnp.where(jnp.logical_not(right) & (onward == d), planes, d)
        return pltpu.make_async_remote_copy(
            src_ref=s_buf.at[d, q],
            dst_ref=s_buf.at[slot, q],
            send_sem=s_send.at[o, q],
            recv_sem=s_recv.at[slot, q],
            device_id={"seq": onward},
            device_id_type=MESH,
        )

    def summed(slot, q):
        return pltpu.make_async_copy(s_buf.at[slot, q], s_buf.at[slot, q], s_recv.at[slot, q])

    def result(q):
        return pltpu.make_async_copy(o_buf.at[q], out.at[:, pl.ds(q * cols, cols)], o_sem.at[q])

    def final(q):
        @pl.when(plane > 0)
        def _():
            summed(plane, q).wait()

        @pl.when(plane < planes - 1)
        def _():
            summed(planes, q).wait()

        @pl.loop(0, rows // block)
        def _(i):
            part = pl.ds(pl.multiple_of(i * block, block), block)
            sides = s_buf[plane, q, part].astype(jnp.float32) + s_buf[planes, q, part].astype(jnp.float32)
            o_buf[q, part] = (acc[q, part] + sides).astype(o_buf.dtype)

        result(q).start()

    def onward(d, o, q):
        @pl.when(jnp.where(d > plane, plane > 0, plane < planes - 1))
        def _():
            summed(d, q).wait()

        @pl.loop(0, rows // block)
        def _(i):
            part = pl.ds(pl.multiple_of(i * block, block), block)
            total = acc[o * parts + q, part] + s_buf[d, q, part].astype(jnp.float32)
            s_buf[d, q, part] = total.astype(s_buf.dtype)

        sum_out(d, o, q).start()

    def settle(by_plane):
        most = max(len(todo) for todo in by_plane.values())
        for turn in range(most):
            todo = [by_plane.get(p, [])[turn : turn + 1] for p in range(planes)]
            d = pick(plane, [t[0][0] if t else -1 for t in todo], -1)
            q = pick(plane, [t[0][1] if t else 0 for t in todo])
            o = pick(plane, [orders[p].index(t[0][0]) if t else 0 for p, t in enumerate(todo)])
            if any(t and t[0][0] == p for p, t in enumerate(todo)):

                @pl.when(d == plane)
                def _():
                    final(q)

            if any(t and t[0][0] != p for p, t in enumerate(todo)):

                @pl.when((d >= 0) & (d != plane))
                def _():
                    onward(d, o, q)

    acc[...] = jnp.zeros_like(acc)

    @pl.when(plane == 0)
    def _():
        for slot in range(planes):
            s_buf[slot] = jnp.zeros(s_buf.shape[1:], s_buf.dtype)

    @pl.when(plane == planes - 1)
    def _():
        for slot in [*range(planes - 1), planes]:
            s_buf[slot] = jnp.zeros(s_buf.shape[1:], s_buf.dtype)

    lanes = lax.broadcasted_iota(jnp.int32, (rows, g_buf.shape[2]), 1)
    firsts = {index: o for o, index in begun.items()}

    @pl.loop(0, len(items))
    def _(index):
        for at in sorted({*events, *firsts, *(k for k in sums if k < len(items))}):

            @pl.when(index == at)
            def _():
                if at in events:
                    arrive(*events[at])
                if at in firsts:
                    meet(firsts[at])
                if at in sums:
                    settle(sums[at])

        code = pick(index, [(o * parts + q) * batches + g for o, q, g in items])
        o, q, g = code // (parts * batches), (code // batches) % parts, code % batches
        d = pick(o, [0] * planes)
        for turn in range(planes):
            d = jnp.where(o == turn, planes_of[turn], d)
        total = acc[o * parts + q]
        for turn in range(BATCH):
            expert = g * BATCH + turn
            gate = jnp.sum(jnp.where(lanes == expert, g_buf[d], 0.0), axis=1, keepdims=True)
            total += gate * jnp.dot(x_buf[d], w_buf[expert, q], preferred_element_type=jnp.float32)
        acc[o * parts + q] = total

    for at in sorted(k for k in sums if k >= len(items)):
        settle(sums[at])
    for q in range(parts):
        result(q).wait()
        for edge in edges:
            pass_on(*edge, q).wait_send()
        for o in range(1, planes):
            sum_out(planes_of[o], o, q).wait_send()
    for o in range(1, planes):
        rows_to(planes_of[o]).wait_send()
        gates_to(planes_of[o]).wait_send()


def fused_buffers(planes, size, tokens, weights):
    local, depth, width = weights.shape
    rows, cols, experts = tokens.shape[0], width // PARTS, local * size
    dma = pltpu.SemaphoreType.DMA
    sends = experts - local
    return [
        pltpu.VMEM((experts, PARTS, depth, cols), jnp.bfloat16),
        pltpu.VMEM((planes, rows, depth), jnp.bfloat16),
        pltpu.VMEM((planes, experts, rows), jnp.float32),
        pltpu.VMEM((planes, rows, experts), jnp.float32),
        pltpu.VMEM((planes * PARTS, rows, cols), jnp.float32),
        pltpu.VMEM((planes + 1, PARTS, rows, cols), jnp.bfloat16),
        pltpu.VMEM((PARTS, rows, cols), jnp.bfloat16),
        dma((local, PARTS)),
        dma((PARTS, sends)),
        dma((experts, PARTS)),
        dma,
        dma((planes,)),
        dma((planes,)),
        dma((planes,)),
        dma((planes,)),
        dma((planes, PARTS)),
        dma((planes + 1, PARTS)),
        dma((PARTS,)),
    ]


def fits(planes, size, tokens, weights):
    local, depth, width = weights.shape
    rows, experts = tokens.shape[0], local * size
    if size & (size - 1) or size < 4 or any(2 * len(group) != BATCH for group in tree(size, local)[0]):
        return False
    held = 2 * experts * depth * width + 2 * planes * rows * depth + 4 * planes * rows * width
    held += 2 * (planes + 2) * rows * width + 4 * planes * rows * (experts + 128)
    return held <= 62 * 2**20


def fused_body(tokens, routes, gates, weights):
    planes, size = lax.axis_size("seq"), lax.axis_size("exp")
    local, depth, width = weights.shape
    rows = tokens.shape[0]
    groups, _ = tree(size, local)
    arrival = [chunk for group in groups for chunk in group + [(delta | 1, own) for delta, own in group]]
    me = lax.axis_index("exp")
    experts = jnp.stack([(me ^ delta) * local + own for delta, own in arrival]).astype(jnp.int32)
    gate = jnp.sum(
        jnp.where(routes.T[None, :, :] == experts[:, None, None], gates.T[None, :, :], 0.0), axis=1
    )
    anywhere = pl.BlockSpec(memory_space=pl.ANY)
    return pl.pallas_call(
        functools.partial(fused_kernel, planes, size),
        out_shape=jax.ShapeDtypeStruct((rows, width), jnp.bfloat16),
        in_specs=[anywhere, anywhere, pl.BlockSpec(memory_space=pltpu.VMEM)],
        out_specs=anywhere,
        scratch_shapes=fused_buffers(planes, size, tokens, weights),
        compiler_params=pltpu.CompilerParams(
            collective_id=0, has_side_effects=True, vmem_limit_bytes=67043328
        ),
    )(tokens, weights, gate)


def body(tokens, routes, gates, weights):
    if fits(lax.axis_size("seq"), lax.axis_size("exp"), tokens, weights):
        return fused_body(tokens, routes, gates, weights)
    return spread_body(tokens, routes, gates, weights)


def solution(mesh):
    return jax.shard_map(
        body,
        mesh=mesh,
        in_specs=(
            P(("seq", "exp"), None),
            P(("seq", "exp"), None),
            P(("seq", "exp"), None),
            P("exp", "seq", None),
        ),
        out_specs=P(("seq", "exp"), None),
        check_vma=False,
    )
```

```python
import functools

import jax
import jax.numpy as jnp
from jax import lax
from jax.experimental import pallas as pl
from jax.experimental.pallas import tpu as pltpu
from jax.sharding import PartitionSpec as P

COLUMN_PARTS = (1, 1)


def project_kernel(per_step, x_ref, gate_ref, w_ref, *rest):
    out_ref = rest[-1]
    step = pl.program_id(0)
    lanes = lax.broadcasted_iota(jnp.int32, gate_ref.shape, 1)

    @pl.when(step == 0)
    def _():
        out_ref[...] = jnp.zeros_like(out_ref)

    total = out_ref[...]
    for own in range(per_step):
        expert = step * per_step + own
        gate = jnp.sum(jnp.where(lanes == expert, gate_ref[...], 0.0), axis=1, keepdims=True)
        total += gate * jnp.dot(x_ref[...], w_ref[own], preferred_element_type=jnp.float32)
    out_ref[...] = total


def project(x, gate, weights, before):
    rows, depth = x.shape
    experts, _, cols = weights.shape
    per_step = 2
    return pl.pallas_call(
        functools.partial(project_kernel, per_step),
        grid=(experts // per_step,),
        out_shape=jax.ShapeDtypeStruct((rows, cols), jnp.float32),
        in_specs=[
            pl.BlockSpec((rows, depth), lambda e: (0, 0)),
            pl.BlockSpec((rows, experts), lambda e: (0, 0)),
            pl.BlockSpec((per_step, depth, cols), lambda e: (e, 0, 0)),
        ]
        + [pl.BlockSpec(memory_space=pl.ANY)] * len(before),
        out_specs=pl.BlockSpec((rows, cols), lambda e: (0, 0)),
        compiler_params=pltpu.CompilerParams(vmem_limit_bytes=32 * 1024 * 1024),
        cost_estimate=pl.CostEstimate(
            flops=2 * rows * depth * cols * experts,
            bytes_accessed=2 * experts * depth * cols + 2 * rows * depth,
            transcendentals=0,
        ),
    )(x, gate, weights, *before)


def shift_order(planes):
    near = [d for pair in zip(range(1, planes), range(planes - 1, 0, -1)) for d in pair]
    return list(dict.fromkeys(near))


def unit_order(planes, parts):
    early = 1
    arrival = [0] + shift_order(planes)
    order = [(d, q) for q in range(early) for d in arrival[:-1]]
    order += [(arrival[-1], q) for q in range(early)]
    for q in range(early, parts):
        order += [(d, q) for d in list(range(1, planes)) + [0]]
    return order


def spread_body(tokens, routes, gates, weights):
    experts = weights.shape[0] * lax.axis_size("exp")
    planes = lax.axis_size("seq")
    plane = lax.axis_index("seq")
    depth = weights.shape[1]
    share = weights.shape[2] // sum(COLUMN_PARTS)
    edges = [share * sum(COLUMN_PARTS[:q]) for q in range(len(COLUMN_PARTS) + 1)]

    def moved(value, shift):
        return lax.ppermute(value, "seq", [(i, (i + shift) % planes) for i in range(planes)])

    def features(target):
        return lax.dynamic_slice_in_dim(tokens, target * depth, depth, 1)

    dense = jnp.sum(
        jnp.where(
            routes[:, None, :] == jnp.arange(experts, dtype=jnp.int32)[None, :, None],
            gates[:, None, :],
            0.0,
        ),
        axis=2,
    )
    sent = dense.T
    gate, x = {0: dense}, {0: features(plane)}
    for shift in range(1, planes):
        gate[shift] = moved(sent, shift).T
    latest = None
    for shift in shift_order(planes):
        piece = features(lax.rem(plane + shift, planes))
        if latest is not None:
            piece, _ = lax.optimization_barrier((piece, latest))
        latest = x[shift] = moved(piece, shift)
    whole = [
        lax.all_gather(weights[:, :, edges[q] : edges[q + 1]], "exp", axis=0, tiled=True)
        for q in range(len(COLUMN_PARTS))
    ]
    parts, running, flying, stage, started = {}, {}, {}, {}, {}
    previous = []
    for index, (shift, q) in enumerate(unit_order(planes, len(COLUMN_PARTS))):
        landed = [key for key in flying if started[key] <= index - 2 and index >= planes]
        done = project(x[shift], gate[shift], whole[q], previous + [flying.pop(key) for key in landed])
        previous = [done]
        parts[shift, q] = done
        at = stage.get(q, 1)
        while at <= planes and (at % planes, q) in parts:
            begin = index
            value = parts[at % planes, q]
            if at > 1:
                value = running[q].astype(jnp.float32) + value
                begin = max(begin, started[at - 1, q] + 1)
            running[q] = value.astype(jnp.bfloat16)
            if at < planes:
                running[q] = moved(running[q], 1)
                flying[at, q] = running[q]
                started[at, q] = begin
            at += 1
        stage[q] = at
    return jnp.concatenate([running[q] for q in range(len(COLUMN_PARTS))], axis=1)


MESH = pl.DeviceIdType.MESH
PARTS = 4
BATCH = 4
STEP, SLOT, WAIT, OVER = 3.15, 12.0, 2.0, 1.5
HOP_EARLY, HOP, FINAL = 16.0, 10.0, 25.0
LANDED = {True: (0.0, 32.0, 65.0, 122.0), False: (0.0, 32.0, 32.0, 95.0)}


def tree(size, local):
    digits = size.bit_length() - 1
    high = list(range(1, digits))

    def order(own):
        turn = own % max(1, len(high))
        return high[turn:] + high[:turn] + [0]

    def last(delta, own):
        return max((order(own).index(b) for b in range(digits) if delta >> b & 1), default=-1)

    def children(delta, own):
        return [b for b in order(own)[last(delta, own) + 1 :]]

    groups = [[(0, own) for own in range(local)]]
    for turn in range(local):
        groups.append([(1 << b, sorted(range(local), key=lambda own: order(own).index(b))[turn]) for b in high])
    for hops in range(2, digits):
        far = [h << 1 for h in range(size // 2) if bin(h).count("1") == hops]
        groups.append([(h, own) for h in far for own in range(local)])
    return groups, children


def line_order(planes):
    middle = (planes - 1) / 2

    def key(p, d):
        hops = abs(d - p)
        return (min(hops, 2), -hops if p in (0, planes - 1) else hops, abs(d - middle), d)

    return [sorted(range(planes), key=functools.partial(key, p)) for p in range(planes)]


def schedule(planes, parts, groups):
    ends = [p in (0, planes - 1) for p in range(planes)]

    def arrival(o, end):
        return LANDED[end][min(o, len(LANDED[end]) - 1)]

    def due(q, g):
        return SLOT * (q * (groups - 1) + g) + WAIT

    def extra(end):
        kind = line_order(planes)[0 if end else 1 % planes]
        tasks = [
            (q, -abs(kind[o] - kind[0]), g, o)
            for q in range(parts)
            for o in range(2, planes)
            for g in range(0, groups, 2)
        ]
        tasks, clock, taken = sorted(tasks), 0.0, {}
        for q in range(parts):
            for g in range(groups):
                clock = max(clock, due(q, g)) + (STEP if q or g % 2 else 0.0)
                if q == 0 and g == groups - 1 and planes > 1:
                    clock = max(clock, arrival(1, end)) + groups // 2 * STEP
                taken[q, g] = []
                follow = due(q, g + 1) if g + 1 < groups else due(q + 1, 0)
                while (q, g) != (parts - 1, groups - 1) and clock + STEP <= follow + OVER:
                    ready = [t for t in tasks if (t[0], t[2] + 1) <= (q, g) and arrival(t[3], end) <= clock]
                    if not ready:
                        break
                    tasks.remove(ready[0])
                    taken[q, g].append((ready[0][3], ready[0][0], ready[0][2]))
                    clock += STEP
        taken["rest"] = [(t[3], t[0], t[2]) for t in tasks]
        return taken

    both = {end: extra(end) for end in (True, False)}
    steps, places = {True: [], False: []}, {}

    def add(work):
        most = max(len(work[end]) for end in work)
        for end in work:
            steps[end] += work[end] + [None] * (most - len(work[end]))

    def halves(work):
        return [((o, q, g), (o, q, g + 1)) for o, q, g in work]

    for q in range(parts):
        for g in range(groups):
            places[q, g] = len(steps[True])
            own = []
            if q == 0:
                if g % 2:
                    own.append(((0, 0, g - 1), (0, 0, g)))
                if g == groups - 1 and planes > 1:
                    own += halves([(1, 0, i) for i in range(0, groups, 2)])
            elif (q, g) != (parts - 1, groups - 1):
                own.append(((0, q, g), (min(1, planes - 1), q, g)))
            add({end: own + halves(both[end][q, g]) for end in both})
    add({end: halves(both[end]["rest"]) for end in both})
    last = ((0, parts - 1, groups - 1), (min(1, planes - 1), parts - 1, groups - 1))
    add({end: [last] for end in both})

    at = {}
    for (q, g), index in places.items():
        at[index] = max(at.get(index, 0.0), due(q, g))
    start, begun, ended = {}, {}, {}
    for end in both:
        clock, start[end] = 0.0, []
        for index, pair in enumerate(steps[end]):
            clock = max([clock, at.get(index, 0.0)] + [arrival(o, end) for o, _, _ in pair or []])
            start[end].append(clock)
            clock += STEP if pair else 0.0
            for o, q, _ in pair or []:
                begun.setdefault((end, o), index)
                ended[end, o, q] = clock
    order = line_order(planes)
    ready = {}
    for q in range(parts):
        for d in range(planes):
            for p in list(range(d)) + list(range(planes - 1, d, -1)) + [d]:
                time = ended[ends[p], order[p].index(d), q]
                before = [p - 1] if p < d else [p + 1] if p > d else [p - 1, p + 1]
                for other in before:
                    if 0 <= other < planes:
                        sent = ready[other, d, q]
                        time = max(time, sent + (HOP_EARLY if sent < LANDED[False][-1] else HOP))
                onward = p + 1 if p < d else p - 1
                if p != d and not ends[p] and not ends[onward]:
                    time = max(time, LANDED[True][-1])
                ready[p, d, q] = time + (FINAL if p == d else 0.0)
    sums = {}
    for p in range(planes):
        end = len(steps[True])
        for time, d, q in sorted((ready[p, d, q], d, q) for d in range(planes) for q in range(parts)):
            where = next((i for i, begin in enumerate(start[ends[p]]) if begin >= time), None)
            if where is None:
                where, end = end, end + 1
            sums.setdefault(where, {}).setdefault(p, []).append((d, q))
    events = {}
    for key, index in places.items():
        events.setdefault(index, []).append(key)
    return steps, events, begun, sums


def pick(which, values, default=0):
    found = jnp.int32(default)
    for index, value in enumerate(values):
        found = jnp.where(which == index, jnp.int32(value), found)
    return found


def fused_kernel(planes, size, tokens, weights, gate_in, out, w_buf, x_buf, t_buf, g_buf, acc, s_buf, o_buf, *sems):
    w_load, w_send, w_recv, x_load, x_send, x_recv, t_send, t_recv, s_send, s_recv, o_sem = sems
    plane, me = lax.axis_index("seq"), lax.axis_index("exp")
    local = weights.shape[0]
    rows, depth = x_buf.shape[1:]
    cols = o_buf.shape[2]
    parts = o_buf.shape[0]
    batches = w_buf.shape[0] // BATCH
    groups, children = tree(size, local)
    arrival = [chunk for group in groups for chunk in group + [(delta | 1, own) for delta, own in group]]
    place = {chunk: index for index, chunk in enumerate(arrival)}
    digits = size.bit_length() - 1
    steps, events, begun, sums = schedule(planes, parts, len(groups))
    orders = line_order(planes)
    at_end = (plane == 0) | (plane == planes - 1)
    planes_of = [pick(plane, [orders[p][o] for p in range(planes)]) for o in range(planes)]
    near = [me + (1 - 2 * (lax.div(me, jnp.int32(1 << b)) % 2)) * (1 << b) for b in range(digits)]

    barrier = pltpu.get_barrier_semaphore()
    own_loads = [
        pltpu.make_async_copy(
            weights.at[own, :, pl.ds(q * cols, cols)], w_buf.at[place[0, own], q], w_load.at[own, q]
        )
        for q in range(parts)
        for own in range(local)
    ]
    own_rows = pltpu.make_async_copy(
        tokens.at[:, pl.ds(pl.multiple_of(plane * depth, depth), depth)], x_buf.at[plane], x_load
    )
    for load in own_loads[:local]:
        load.start()
    own_rows.start()
    for load in own_loads[local:]:
        load.start()
    for b in range(digits):
        pl.semaphore_signal(barrier, inc=1, device_id={"exp": near[b]}, device_id_type=MESH)
    for shift in range(1, planes):
        pl.semaphore_signal(
            barrier, inc=1, device_id={"seq": lax.rem(plane + shift, planes)}, device_id_type=MESH
        )
    pl.semaphore_wait(barrier, digits + planes - 1)

    def rows_to(target):
        return pltpu.make_async_remote_copy(
            src_ref=tokens.at[:, pl.ds(pl.multiple_of(target * depth, depth), depth)],
            dst_ref=x_buf.at[plane],
            send_sem=x_send.at[target],
            recv_sem=x_recv.at[plane],
            device_id={"seq": target},
            device_id_type=MESH,
        )

    def gates_to(target):
        return pltpu.make_async_remote_copy(
            src_ref=gate_in,
            dst_ref=t_buf.at[plane],
            send_sem=t_send.at[target],
            recv_sem=t_recv.at[plane],
            device_id={"seq": target},
            device_id_type=MESH,
        )

    def spread(distance, outer):
        for target in (plane + distance, plane - distance):
            end = (target == 0) | (target == planes - 1)

            @pl.when((target >= 0) & (target < planes) & (end if outer else jnp.logical_not(end)))
            def _():
                gates_to(target).start()
                rows_to(target).start()

    far = [(distance, outer) for distance in range(3, planes) for outer in (True, False)]
    leave = {
        (0, 0): [(1, True), (1, False)],
        (0, len(groups) - 1): far,
        (parts - 3, 2): [(2, False)],
        (parts - 2, 2): [(2, True)],
    }
    sent = []

    def pass_on(delta, own, b, q):
        copy = pltpu.make_async_remote_copy(
            src_ref=w_buf.at[place[delta, own], q],
            dst_ref=w_buf.at[place[delta ^ (1 << b), own], q],
            send_sem=w_send.at[q, count(delta, own, b)],
            recv_sem=w_recv.at[place[delta ^ (1 << b), own], q],
            device_id={"exp": near[b]},
            device_id_type=MESH,
        )
        return copy

    edges = [(delta, own, b) for group in groups for delta, own in group for b in children(delta, own)]

    def count(*edge):
        return edges.index(edge)

    def send_own(q):
        for own in range(local):
            own_loads[q * local + own].wait()
        for group in groups[1 : local + 1]:
            for delta, own in group:
                pass_on(0, own, delta.bit_length() - 1, q).start()
        for own in range(local):
            pass_on(0, own, 0, q).start()

    def landing(chunk, q):
        index = place[chunk]
        return pltpu.make_async_copy(w_buf.at[index, q], w_buf.at[index, q], w_recv.at[index, q])

    def arrive(q, g):
        if g == 0 and q == 0:
            send_own(0)
        for distance, outer in leave.get((q, g), []):
            if distance < planes:
                spread(distance, outer)
        if g > 0:
            for delta, own in groups[g]:
                landing((delta, own), q).wait()
                for b in children(delta, own):
                    pass_on(delta, own, b, q).start()
        if g == len(groups) - 2 and q + 1 < parts:
            send_own(q + 1)
        if (q, g) == (0, 0):
            clear()
        for delta, own in groups[g]:
            landing((delta | 1, own), q).wait()

    def clear():
        acc[...] = jnp.zeros_like(acc)

        @pl.when(plane == 0)
        def _():
            for slot in range(planes):
                s_buf[slot] = jnp.zeros(s_buf.shape[1:], s_buf.dtype)

        @pl.when(plane == planes - 1)
        def _():
            for slot in [*range(planes - 1), planes]:
                s_buf[slot] = jnp.zeros(s_buf.shape[1:], s_buf.dtype)

    def meet(o):
        d = planes_of[o]
        if o == 0:
            own_rows.wait()
            g_buf[d] = gate_in[...].T
        else:
            pltpu.make_async_copy(x_buf.at[d], x_buf.at[d], x_recv.at[d]).wait()
            pltpu.make_async_copy(t_buf.at[d], t_buf.at[d], t_recv.at[d]).wait()
            g_buf[d] = t_buf[d].T

    block = 64 if rows % 64 == 0 else rows

    def sum_out(d, o, q):
        right = d > plane
        onward = jnp.where(right, plane + 1, plane - 1)
        slot = jnp.where(jnp.logical_not(right) & (onward == d), planes, d)
        return pltpu.make_async_remote_copy(
            src_ref=s_buf.at[d, q],
            dst_ref=s_buf.at[slot, q],
            send_sem=s_send.at[o, q],
            recv_sem=s_recv.at[slot, q],
            device_id={"seq": onward},
            device_id_type=MESH,
        )

    def summed(slot, q):
        return pltpu.make_async_copy(s_buf.at[slot, q], s_buf.at[slot, q], s_recv.at[slot, q])

    def result(q):
        return pltpu.make_async_copy(o_buf.at[q], out.at[:, pl.ds(q * cols, cols)], o_sem.at[q])

    def final(q):
        @pl.when(plane > 0)
        def _():
            summed(plane, q).wait()

        @pl.when(plane < planes - 1)
        def _():
            summed(planes, q).wait()

        @pl.loop(0, rows // block)
        def _(i):
            part = pl.ds(pl.multiple_of(i * block, block), block)
            sides = s_buf[plane, q, part].astype(jnp.float32) + s_buf[planes, q, part].astype(jnp.float32)
            o_buf[q, part] = (acc[q, part] + sides).astype(o_buf.dtype)

        result(q).start()

    def onward(d, o, q):
        @pl.when(jnp.where(d > plane, plane > 0, plane < planes - 1))
        def _():
            summed(d, q).wait()

        @pl.loop(0, rows // block)
        def _(i):
            part = pl.ds(pl.multiple_of(i * block, block), block)
            total = acc[o * parts + q, part] + s_buf[d, q, part].astype(jnp.float32)
            s_buf[d, q, part] = total.astype(s_buf.dtype)

        sum_out(d, o, q).start()

    def settle(by_plane):
        most = max(len(todo) for todo in by_plane.values())
        for turn in range(most):
            todo = [by_plane.get(p, [])[turn : turn + 1] for p in range(planes)]
            d = pick(plane, [t[0][0] if t else -1 for t in todo], -1)
            q = pick(plane, [t[0][1] if t else 0 for t in todo])
            o = pick(plane, [orders[p].index(t[0][0]) if t else 0 for p, t in enumerate(todo)])
            if any(t and t[0][0] == p for p, t in enumerate(todo)):

                @pl.when(d == plane)
                def _():
                    final(q)

            if any(t and t[0][0] != p for p, t in enumerate(todo)):

                @pl.when((d >= 0) & (d != plane))
                def _():
                    onward(d, o, q)

    lanes = lax.broadcasted_iota(jnp.int32, (rows, g_buf.shape[2]), 1)
    def before(index, at):
        @pl.when(index == at)
        def _():
            for key in events.get(at, []):
                arrive(*key)
            for (end, o), index_of in begun.items():
                if index_of == at and begun[not end, o] == at:
                    if end:
                        meet(o)
                elif index_of == at:

                    @pl.when(at_end if end else jnp.logical_not(at_end))
                    def _():
                        meet(o)
            if at in sums:
                settle(sums[at])

    def search(index, points):
        if len(points) == 1:
            before(index, points[0])
        elif points:
            half = len(points) // 2

            @pl.when(index < points[half])
            def _():
                search(index, points[:half])

            @pl.when(index >= points[half])
            def _():
                search(index, points[half:])

    def products(code):
        o, q, g = code // (parts * batches), (code // batches) % parts, code % batches
        d = pick(o, [0])
        for turn in range(planes):
            d = jnp.where(o == turn, planes_of[turn], d)
        total = None
        for turn in range(BATCH):
            expert = g * BATCH + turn
            gate = jnp.sum(jnp.where(lanes == expert, g_buf[d], 0.0), axis=1, keepdims=True)
            term = gate * jnp.dot(x_buf[d], w_buf[expert, q], preferred_element_type=jnp.float32)
            total = term if total is None else total + term
        acc[o * parts + q] += total

    def code_of(pair, side):
        if pair is None:
            return -1
        o, q, g = pair[side]
        return (o * parts + q) * batches + g

    total_steps = len(steps[True])
    points = sorted({*events, *begun.values(), *(k for k in sums if k < total_steps)})

    @pl.loop(0, total_steps)
    def _(index):
        search(index, points)
        codes = []
        for side in range(2):
            ways = [pick(index, [code_of(pair, side) for pair in steps[end]]) for end in (True, False)]
            codes.append(jnp.where(at_end, *ways))

        @pl.when(codes[0] >= 0)
        def _():
            for code in codes:
                products(code)

    for at in sorted(k for k in sums if k >= total_steps):
        settle(sums[at])
    for q in range(parts):
        result(q).wait()
        for edge in edges:
            pass_on(*edge, q).wait_send()
        for o in range(1, planes):
            sum_out(planes_of[o], o, q).wait_send()
    for o in range(1, planes):
        rows_to(planes_of[o]).wait_send()
        gates_to(planes_of[o]).wait_send()


def fused_buffers(planes, size, tokens, weights):
    local, depth, width = weights.shape
    rows, cols, experts = tokens.shape[0], width // PARTS, local * size
    dma = pltpu.SemaphoreType.DMA
    sends = experts - local
    return [
        pltpu.VMEM((experts, PARTS, depth, cols), jnp.bfloat16),
        pltpu.VMEM((planes, rows, depth), jnp.bfloat16),
        pltpu.VMEM((planes, experts, rows), jnp.float32),
        pltpu.VMEM((planes, rows, experts), jnp.float32),
        pltpu.VMEM((planes * PARTS, rows, cols), jnp.float32),
        pltpu.VMEM((planes + 1, PARTS, rows, cols), jnp.bfloat16),
        pltpu.VMEM((PARTS, rows, cols), jnp.bfloat16),
        dma((local, PARTS)),
        dma((PARTS, sends)),
        dma((experts, PARTS)),
        dma,
        dma((planes,)),
        dma((planes,)),
        dma((planes,)),
        dma((planes,)),
        dma((planes, PARTS)),
        dma((planes + 1, PARTS)),
        dma((PARTS,)),
    ]


def fits(planes, size, tokens, weights):
    local, depth, width = weights.shape
    rows, experts = tokens.shape[0], local * size
    if size & (size - 1) or size < 4 or any(2 * len(group) != BATCH for group in tree(size, local)[0]):
        return False
    held = 2 * experts * depth * width + 2 * planes * rows * depth + 4 * planes * rows * width
    held += 2 * (planes + 2) * rows * width + 4 * planes * rows * (experts + 128)
    return held <= 62 * 2**20


def fused_body(tokens, routes, gates, weights):
    planes, size = lax.axis_size("seq"), lax.axis_size("exp")
    local, depth, width = weights.shape
    rows = tokens.shape[0]
    groups, _ = tree(size, local)
    arrival = [chunk for group in groups for chunk in group + [(delta | 1, own) for delta, own in group]]
    me = lax.axis_index("exp")
    experts = jnp.stack([(me ^ delta) * local + own for delta, own in arrival]).astype(jnp.int32)
    gate = jnp.sum(
        jnp.where(routes.T[None, :, :] == experts[:, None, None], gates.T[None, :, :], 0.0), axis=1
    )
    anywhere = pl.BlockSpec(memory_space=pl.ANY)
    return pl.pallas_call(
        functools.partial(fused_kernel, planes, size),
        out_shape=jax.ShapeDtypeStruct((rows, width), jnp.bfloat16),
        in_specs=[anywhere, anywhere, pl.BlockSpec(memory_space=pltpu.VMEM)],
        out_specs=anywhere,
        scratch_shapes=fused_buffers(planes, size, tokens, weights),
        compiler_params=pltpu.CompilerParams(
            collective_id=0, has_side_effects=True, vmem_limit_bytes=67043328
        ),
    )(tokens, weights, gate)


def body(tokens, routes, gates, weights):
    if fits(lax.axis_size("seq"), lax.axis_size("exp"), tokens, weights):
        return fused_body(tokens, routes, gates, weights)
    return spread_body(tokens, routes, gates, weights)


def solution(mesh):
    return jax.shard_map(
        body,
        mesh=mesh,
        in_specs=(
            P(("seq", "exp"), None),
            P(("seq", "exp"), None),
            P(("seq", "exp"), None),
            P("exp", "seq", None),
        ),
        out_specs=P(("seq", "exp"), None),
        check_vma=False,
    )
```

```python
import functools

import jax
import jax.numpy as jnp
from jax import lax
from jax.experimental import pallas as pl
from jax.experimental.pallas import tpu as pltpu
from jax.sharding import PartitionSpec as P

COLUMN_PARTS = (1, 1)


def project_kernel(per_step, x_ref, gate_ref, w_ref, *rest):
    out_ref = rest[-1]
    step = pl.program_id(0)
    lanes = lax.broadcasted_iota(jnp.int32, gate_ref.shape, 1)

    @pl.when(step == 0)
    def _():
        out_ref[...] = jnp.zeros_like(out_ref)

    total = out_ref[...]
    for own in range(per_step):
        expert = step * per_step + own
        gate = jnp.sum(jnp.where(lanes == expert, gate_ref[...], 0.0), axis=1, keepdims=True)
        total += gate * jnp.dot(x_ref[...], w_ref[own], preferred_element_type=jnp.float32)
    out_ref[...] = total


def project(x, gate, weights, before):
    rows, depth = x.shape
    experts, _, cols = weights.shape
    per_step = 2
    return pl.pallas_call(
        functools.partial(project_kernel, per_step),
        grid=(experts // per_step,),
        out_shape=jax.ShapeDtypeStruct((rows, cols), jnp.float32),
        in_specs=[
            pl.BlockSpec((rows, depth), lambda e: (0, 0)),
            pl.BlockSpec((rows, experts), lambda e: (0, 0)),
            pl.BlockSpec((per_step, depth, cols), lambda e: (e, 0, 0)),
        ]
        + [pl.BlockSpec(memory_space=pl.ANY)] * len(before),
        out_specs=pl.BlockSpec((rows, cols), lambda e: (0, 0)),
        compiler_params=pltpu.CompilerParams(vmem_limit_bytes=32 * 1024 * 1024),
        cost_estimate=pl.CostEstimate(
            flops=2 * rows * depth * cols * experts,
            bytes_accessed=2 * experts * depth * cols + 2 * rows * depth,
            transcendentals=0,
        ),
    )(x, gate, weights, *before)


def shift_order(planes):
    near = [d for pair in zip(range(1, planes), range(planes - 1, 0, -1)) for d in pair]
    return list(dict.fromkeys(near))


def unit_order(planes, parts):
    early = 1
    arrival = [0] + shift_order(planes)
    order = [(d, q) for q in range(early) for d in arrival[:-1]]
    order += [(arrival[-1], q) for q in range(early)]
    for q in range(early, parts):
        order += [(d, q) for d in list(range(1, planes)) + [0]]
    return order


def spread_body(tokens, routes, gates, weights):
    experts = weights.shape[0] * lax.axis_size("exp")
    planes = lax.axis_size("seq")
    plane = lax.axis_index("seq")
    depth = weights.shape[1]
    share = weights.shape[2] // sum(COLUMN_PARTS)
    edges = [share * sum(COLUMN_PARTS[:q]) for q in range(len(COLUMN_PARTS) + 1)]

    def moved(value, shift):
        return lax.ppermute(value, "seq", [(i, (i + shift) % planes) for i in range(planes)])

    def features(target):
        return lax.dynamic_slice_in_dim(tokens, target * depth, depth, 1)

    dense = jnp.sum(
        jnp.where(
            routes[:, None, :] == jnp.arange(experts, dtype=jnp.int32)[None, :, None],
            gates[:, None, :],
            0.0,
        ),
        axis=2,
    )
    sent = dense.T
    gate, x = {0: dense}, {0: features(plane)}
    for shift in range(1, planes):
        gate[shift] = moved(sent, shift).T
    latest = None
    for shift in shift_order(planes):
        piece = features(lax.rem(plane + shift, planes))
        if latest is not None:
            piece, _ = lax.optimization_barrier((piece, latest))
        latest = x[shift] = moved(piece, shift)
    whole = [
        lax.all_gather(weights[:, :, edges[q] : edges[q + 1]], "exp", axis=0, tiled=True)
        for q in range(len(COLUMN_PARTS))
    ]
    parts, running, flying, stage, started = {}, {}, {}, {}, {}
    previous = []
    for index, (shift, q) in enumerate(unit_order(planes, len(COLUMN_PARTS))):
        landed = [key for key in flying if started[key] <= index - 2 and index >= planes]
        done = project(x[shift], gate[shift], whole[q], previous + [flying.pop(key) for key in landed])
        previous = [done]
        parts[shift, q] = done
        at = stage.get(q, 1)
        while at <= planes and (at % planes, q) in parts:
            begin = index
            value = parts[at % planes, q]
            if at > 1:
                value = running[q].astype(jnp.float32) + value
                begin = max(begin, started[at - 1, q] + 1)
            running[q] = value.astype(jnp.bfloat16)
            if at < planes:
                running[q] = moved(running[q], 1)
                flying[at, q] = running[q]
                started[at, q] = begin
            at += 1
        stage[q] = at
    return jnp.concatenate([running[q] for q in range(len(COLUMN_PARTS))], axis=1)


MESH = pl.DeviceIdType.MESH
PARTS = 4
BATCH = 4
HALVES = 2
STEP, SLOT, WAIT, OVER = 3.15, 12.0, 2.0, 1.5
HOP_EARLY, HOP, ACROSS, FINAL = 16.0, 10.0, 15.0, 25.0
LANDED = {True: (0.0, 32.0, 62.0, 124.0), False: (0.0, 32.0, 32.0, 97.0)}


def tree(size, local):
    digits = size.bit_length() - 1
    high = list(range(1, digits))

    def order(own):
        turn = own % max(1, len(high))
        return high[turn:] + high[:turn] + [0]

    def last(delta, own):
        return max((order(own).index(b) for b in range(digits) if delta >> b & 1), default=-1)

    def children(delta, own):
        return [b for b in order(own)[last(delta, own) + 1 :]]

    groups = [[(0, own) for own in range(local)]]
    for turn in range(local):
        groups.append([(1 << b, sorted(range(local), key=lambda own: order(own).index(b))[turn]) for b in high])
    for hops in range(2, digits):
        far = [h << 1 for h in range(size // 2) if bin(h).count("1") == hops]
        groups.append([(h, own) for h in far for own in range(local)])
    return groups, children


def line_order(planes):
    middle = (planes - 1) / 2

    def key(p, d):
        hops = abs(d - p)
        return (min(hops, 2), -hops if p in (0, planes - 1) else hops, abs(d - middle), d)

    return [sorted(range(planes), key=functools.partial(key, p)) for p in range(planes)]


def schedule(planes, parts, groups):
    ends = [p in (0, planes - 1) for p in range(planes)]

    def arrival(o, end):
        return LANDED[end][min(o, len(LANDED[end]) - 1)]

    def due(q, g):
        return SLOT * (q * (groups - 1) + g) + WAIT

    def extra(end):
        kind = line_order(planes)[0 if end else 1 % planes]
        tasks = [
            (q, -abs(kind[o] - kind[0]), g, o)
            for q in range(parts)
            for o in range(2, planes)
            for g in range(0, groups, 2)
        ]
        tasks, clock, taken = sorted(tasks), 0.0, {}
        for q in range(parts):
            for g in range(groups):
                clock = max(clock, due(q, g)) + (STEP if q or g % 2 else 0.0)
                if q == 0 and g == groups - 1 and planes > 1:
                    clock = max(clock, arrival(1, end)) + groups // 2 * STEP
                taken[q, g] = []
                follow = due(q, g + 1) if g + 1 < groups else due(q + 1, 0)
                while (q, g) != (parts - 1, groups - 1) and clock + STEP <= follow + OVER:
                    ready = [t for t in tasks if (t[0], t[2] + 1) <= (q, g) and arrival(t[3], end) <= clock]
                    if not ready:
                        break
                    tasks.remove(ready[0])
                    taken[q, g].append((ready[0][3], ready[0][0], ready[0][2]))
                    clock += STEP
        taken["rest"] = [(t[3], t[0], t[2]) for t in tasks]
        return taken

    both = {end: extra(end) for end in (True, False)}
    steps, places = {True: [], False: []}, {}

    def add(work):
        most = max(len(work[end]) for end in work)
        for end in work:
            steps[end] += work[end] + [None] * (most - len(work[end]))

    def halves(work):
        return [((o, q, g), (o, q, g + 1)) for o, q, g in work]

    for q in range(parts):
        for g in range(groups):
            places[q, g] = len(steps[True])
            own = []
            if q == 0:
                if g % 2:
                    own.append(((0, 0, g - 1), (0, 0, g)))
                if g == groups - 1 and planes > 1:
                    own += halves([(1, 0, i) for i in range(0, groups, 2)])
            elif (q, g) != (parts - 1, groups - 1):
                own.append(((0, q, g), (min(1, planes - 1), q, g)))
            add({end: own + halves(both[end][q, g]) for end in both})
    add({end: halves(both[end]["rest"]) for end in both})
    last = ((0, parts - 1, groups - 1), (min(1, planes - 1), parts - 1, groups - 1))
    add({end: [last] for end in both})

    at = {}
    for (q, g), index in places.items():
        at[index] = max(at.get(index, 0.0), due(q, g))
    start, begun, ended = {}, {}, {}
    for end in both:
        clock, start[end] = 0.0, []
        for index, pair in enumerate(steps[end]):
            clock = max([clock, at.get(index, 0.0)] + [arrival(o, end) for o, _, _ in pair or []])
            start[end].append(clock)
            clock += STEP if pair else 0.0
            for o, q, _ in pair or []:
                begun.setdefault((end, o), index)
                ended[end, o, q] = clock
    order = line_order(planes)
    ready = {}
    for q in range(parts):
        for d in range(planes):
            for p in list(range(d)) + list(range(planes - 1, d, -1)) + [d]:
                time = ended[ends[p], order[p].index(d), q]
                before = [p - 1] if p < d else [p + 1] if p > d else [p - 1, p + 1]
                for other in before:
                    if 0 <= other < planes:
                        sent = ready[other, d, q]
                        hop = HOP_EARLY if sent < LANDED[False][-1] else HOP
                        time = max(time, sent + (hop if ends[p] or ends[other] else ACROSS))
                onward = p + 1 if p < d else p - 1
                if p != d and not ends[p] and not ends[onward]:
                    time = max(time, LANDED[True][-1])
                ready[p, d, q] = time + (FINAL if p == d else 0.0)
    sums = {}
    for p in range(planes):
        end = len(steps[True])
        for time, d, q in sorted((ready[p, d, q], d, q) for d in range(planes) for q in range(parts)):
            where = next((i for i, begin in enumerate(start[ends[p]]) if begin >= time), None)
            if where is None:
                where, end = end, end + 1
            sums.setdefault(where, {}).setdefault(p, []).append((d, q))
    events = {}
    for key, index in places.items():
        events.setdefault(index, []).append(key)
    return steps, events, begun, sums


def pick(which, values, default=0):
    found = jnp.int32(default)
    for index, value in enumerate(values):
        found = jnp.where(which == index, jnp.int32(value), found)
    return found


def fused_kernel(planes, size, tokens, weights, routes, gates, out, *scratch):
    w_buf, x_buf, r_buf, v_buf, t_buf, g_buf, acc, s_buf = scratch[:8]
    w_load, w_send, w_recv, x_load, r_load, x_send, x_recv, t_send, t_recv, s_send, s_recv = scratch[8:]
    plane, me = lax.axis_index("seq"), lax.axis_index("exp")
    local = weights.shape[0]
    rows, depth = x_buf.shape[1:]
    parts, cols = w_buf.shape[1], w_buf.shape[3]
    halves = s_recv.shape[2]
    batches = w_buf.shape[0] // BATCH
    groups, children = tree(size, local)
    arrival = [chunk for group in groups for chunk in group + [(delta | 1, own) for delta, own in group]]
    place = {chunk: index for index, chunk in enumerate(arrival)}
    digits = size.bit_length() - 1
    steps, events, begun, sums = schedule(planes, parts, len(groups))
    orders = line_order(planes)
    at_end = (plane == 0) | (plane == planes - 1)
    planes_of = [pick(plane, [orders[p][o] for p in range(planes)]) for o in range(planes)]
    near = [me + (1 - 2 * (lax.div(me, jnp.int32(1 << b)) % 2)) * (1 << b) for b in range(digits)]

    barrier = pltpu.get_barrier_semaphore()
    own_loads = [
        pltpu.make_async_copy(
            weights.at[own, :, pl.ds(q * cols, cols)], w_buf.at[place[0, own], q], w_load.at[own, q]
        )
        for q in range(parts)
        for own in range(local)
    ]
    own_rows = pltpu.make_async_copy(
        tokens.at[:, pl.ds(pl.multiple_of(plane * depth, depth), depth)], x_buf.at[plane], x_load
    )
    small = [pltpu.make_async_copy(routes, r_buf, r_load.at[0]), pltpu.make_async_copy(gates, v_buf, r_load.at[1])]
    for load in own_loads[:local] + small:
        load.start()
    for b in range(digits):
        pl.semaphore_signal(barrier, inc=1, device_id={"exp": near[b]}, device_id_type=MESH)
    for shift in range(1, planes):
        pl.semaphore_signal(
            barrier, inc=1, device_id={"seq": lax.rem(plane + shift, planes)}, device_id_type=MESH
        )
    pl.semaphore_wait(barrier, digits + planes - 1)

    def rows_to(target):
        return pltpu.make_async_remote_copy(
            src_ref=tokens.at[:, pl.ds(pl.multiple_of(target * depth, depth), depth)],
            dst_ref=x_buf.at[plane],
            send_sem=x_send.at[target],
            recv_sem=x_recv.at[plane],
            device_id={"seq": target},
            device_id_type=MESH,
        )

    def gates_to(target):
        return pltpu.make_async_remote_copy(
            src_ref=t_buf.at[plane],
            dst_ref=t_buf.at[plane],
            send_sem=t_send.at[target],
            recv_sem=t_recv.at[plane],
            device_id={"seq": target},
            device_id_type=MESH,
        )

    def spread(distance, outer):
        for target in (plane + distance, plane - distance):
            end = (target == 0) | (target == planes - 1)

            @pl.when((target >= 0) & (target < planes) & (end if outer else jnp.logical_not(end)))
            def _():
                rows_to(target).start()

    far = [(distance, outer) for distance in range(3, planes) for outer in (True, False)]
    leave = {
        (0, 0): [(1, True), (1, False)],
        (0, len(groups) - 1): far,
        (parts - 3, 2): [(2, False)],
        (parts - 2, 1): [(2, True)],
    }
    sent = []

    def pass_on(delta, own, b, q):
        copy = pltpu.make_async_remote_copy(
            src_ref=w_buf.at[place[delta, own], q],
            dst_ref=w_buf.at[place[delta ^ (1 << b), own], q],
            send_sem=w_send.at[q, count(delta, own, b)],
            recv_sem=w_recv.at[place[delta ^ (1 << b), own], q],
            device_id={"exp": near[b]},
            device_id_type=MESH,
        )
        return copy

    edges = [(delta, own, b) for group in groups for delta, own in group for b in children(delta, own)]

    def count(*edge):
        return edges.index(edge)

    def send_own(q):
        for own in range(local):
            own_loads[q * local + own].wait()
        for group in groups[1 : local + 1]:
            for delta, own in group:
                pass_on(0, own, delta.bit_length() - 1, q).start()
        for own in range(local):
            pass_on(0, own, 0, q).start()

    def landing(chunk, q):
        index = place[chunk]
        return pltpu.make_async_copy(w_buf.at[index, q], w_buf.at[index, q], w_recv.at[index, q])

    def arrive(q, g):
        for distance, outer in leave.get((q, g), []):
            if distance < planes:
                spread(distance, outer)
        if g == 0 and q == 0:
            send_own(0)
            own_rows.start()
            for load in own_loads[local:]:
                load.start()
            clear()
            own_gates()
        if g > 0:
            for delta, own in groups[g]:
                landing((delta, own), q).wait()
                for b in children(delta, own):
                    pass_on(delta, own, b, q).start()
        if (q, g) == (0, 1):
            for turn in range(1, planes):
                gates_to(planes_of[turn]).start()
        if g == len(groups) - 2 and q + 1 < parts:
            send_own(q + 1)
        for delta, own in groups[g]:
            landing((delta | 1, own), q).wait()

    def own_gates():
        for load in small:
            load.wait()
        row = lax.broadcasted_iota(jnp.int32, t_buf.shape[1:], 0)
        expert = jnp.zeros(t_buf.shape[1:], jnp.int32)
        for index, (delta, own) in enumerate(arrival):
            source = me + sum(near[b] - me for b in range(digits) if delta >> b & 1)
            expert = jnp.where(row == index, source * local + own, expert)
        t_buf[plane] = sum(
            jnp.where(r_buf[k : k + 1, :] == expert, v_buf[k : k + 1, :], 0.0) for k in range(r_buf.shape[0])
        )

    def clear():
        acc[...] = jnp.zeros_like(acc)

        @pl.when(plane == 0)
        def _():
            for slot in range(planes):
                s_buf[slot] = jnp.zeros(s_buf.shape[1:], s_buf.dtype)

        @pl.when(plane == planes - 1)
        def _():
            for slot in [*range(planes - 1), planes]:
                s_buf[slot] = jnp.zeros(s_buf.shape[1:], s_buf.dtype)

    def meet(o):
        d = planes_of[o]
        if o == 0:
            own_rows.wait()
            g_buf[d] = t_buf[d].T
        else:
            pltpu.make_async_copy(x_buf.at[d], x_buf.at[d], x_recv.at[d]).wait()
            pltpu.make_async_copy(t_buf.at[d], t_buf.at[d], t_recv.at[d]).wait()
            g_buf[d] = t_buf[d].T

    span = rows // halves
    block = 64 if span % 64 == 0 else span

    def sum_out(d, o, q, half):
        right = d > plane
        onward = jnp.where(right, plane + 1, plane - 1)
        slot = jnp.where(jnp.logical_not(right) & (onward == d), planes, d)
        part = pl.ds(half * span, span)
        return pltpu.make_async_remote_copy(
            src_ref=s_buf.at[d, q, part],
            dst_ref=s_buf.at[slot, q, part],
            send_sem=s_send.at[o, q, half],
            recv_sem=s_recv.at[slot, q, half],
            device_id={"seq": onward},
            device_id_type=MESH,
        )

    def summed(slot, q, half):
        part = s_buf.at[slot, q, pl.ds(half * span, span)]
        return pltpu.make_async_copy(part, part, s_recv.at[slot, q, half])

    def final(q):
        for half in range(halves):

            @pl.when(plane > 0)
            def _():
                summed(plane, q, half).wait()

            @pl.when(plane < planes - 1)
            def _():
                summed(planes, q, half).wait()

            @pl.loop(half * span // block, (half + 1) * span // block)
            def _(i):
                part = pl.ds(pl.multiple_of(i * block, block), block)
                sides = s_buf[plane, q, part].astype(jnp.float32) + s_buf[planes, q, part].astype(jnp.float32)
                total = acc[q, part] + sides
                out[part, pl.ds(pl.multiple_of(q * cols, cols), cols)] = total.astype(out.dtype)

    def onward(d, o, q, ahead):
        for half in range(halves):
            if ahead is not None:

                @pl.when(ahead[0] >= 0)
                def _():
                    sum_out(*ahead, half).wait_send()


            @pl.when(jnp.where(d > plane, plane > 0, plane < planes - 1))
            def _():
                summed(d, q, half).wait()

            @pl.loop(half * span // block, (half + 1) * span // block)
            def _(i):
                part = pl.ds(pl.multiple_of(i * block, block), block)
                total = acc[o * parts + q, part] + s_buf[d, q, part].astype(jnp.float32)
                s_buf[d, q, part] = total.astype(s_buf.dtype)

            sum_out(d, o, q, half).start()

    total_steps = len(steps[True])
    waited = {}

    def behind(p, index, d):
        way = [k for k in range(total_steps, index) for e, _ in sums.get(k, {}).get(p, []) if e != p and (e > p) == (d > p)]
        return next(t for t in sums[way[-1]][p]) if way else None

    def settle(index):
        by_plane = sums[index]
        most = max(len(todo) for todo in by_plane.values())
        for turn in range(most):
            todo = [by_plane.get(p, [])[turn : turn + 1] for p in range(planes)]
            d = pick(plane, [t[0][0] if t else -1 for t in todo], -1)
            q = pick(plane, [t[0][1] if t else 0 for t in todo])
            o = pick(plane, [orders[p].index(t[0][0]) if t else 0 for p, t in enumerate(todo)])
            if any(t and t[0][0] == p for p, t in enumerate(todo)):

                @pl.when(d == plane)
                def _():
                    final(q)

            if any(t and t[0][0] != p for p, t in enumerate(todo)):
                ahead = [behind(p, index, t[0][0]) if t and t[0][0] != p else None for p, t in enumerate(todo)]
                for p, a in enumerate(ahead):
                    if a:
                        waited.setdefault((orders[p].index(a[0]), a[1]), []).append(p)
                before_it = None
                if any(ahead):
                    before_it = (
                        pick(plane, [a[0] if a else -1 for a in ahead], -1),
                        pick(plane, [orders[p].index(a[0]) if a else 0 for p, a in enumerate(ahead)]),
                        pick(plane, [a[1] if a else 0 for a in ahead]),
                    )

                @pl.when((d >= 0) & (d != plane))
                def _():
                    onward(d, o, q, before_it)

    lanes = lax.broadcasted_iota(jnp.int32, (rows, g_buf.shape[2]), 1)
    def before(index, at):
        @pl.when(index == at)
        def _():
            for key in events.get(at, []):
                arrive(*key)
            for (end, o), index_of in begun.items():
                if index_of == at and begun[not end, o] == at:
                    if end:
                        meet(o)
                elif index_of == at:

                    @pl.when(at_end if end else jnp.logical_not(at_end))
                    def _():
                        meet(o)
            if at in sums:
                settle(at)

    def search(index, points):
        if len(points) == 1:
            before(index, points[0])
        elif points:
            half = len(points) // 2

            @pl.when(index < points[half])
            def _():
                search(index, points[:half])

            @pl.when(index >= points[half])
            def _():
                search(index, points[half:])

    def products(code):
        o, q, g = code // (parts * batches), (code // batches) % parts, code % batches
        d = pick(o, [0])
        for turn in range(planes):
            d = jnp.where(o == turn, planes_of[turn], d)
        total = None
        for turn in range(BATCH):
            expert = g * BATCH + turn
            gate = jnp.sum(jnp.where(lanes == expert, g_buf[d], 0.0), axis=1, keepdims=True)
            term = gate * jnp.dot(x_buf[d], w_buf[expert, q], preferred_element_type=jnp.float32)
            total = term if total is None else total + term
        acc[o * parts + q] += total

    def code_of(pair, side):
        if pair is None:
            return -1
        o, q, g = pair[side]
        return (o * parts + q) * batches + g

    points = sorted({*events, *begun.values(), *(k for k in sums if k < total_steps)})

    @pl.loop(0, total_steps)
    def _(index):
        search(index, points)
        codes = []
        for side in range(2):
            ways = [pick(index, [code_of(pair, side) for pair in steps[end]]) for end in (True, False)]
            codes.append(jnp.where(at_end, *ways))

        @pl.when(codes[0] >= 0)
        def _():
            for code in codes:
                products(code)

    for at in sorted(k for k in sums if k >= total_steps):
        settle(at)
    for q in range(parts):
        for edge in edges:
            pass_on(*edge, q).wait_send()
        for o in range(1, planes):
            left = jnp.bool_(True)
            for p in waited.get((o, q), []):
                left = left & (plane != p)

            @pl.when(left)
            def _():
                for half in range(halves):
                    sum_out(planes_of[o], o, q, half).wait_send()

    for o in range(1, planes):
        rows_to(planes_of[o]).wait_send()
        gates_to(planes_of[o]).wait_send()


def fused_buffers(planes, size, tokens, weights):
    local, depth, width = weights.shape
    rows, cols, experts = tokens.shape[0], width // PARTS, local * size
    dma = pltpu.SemaphoreType.DMA
    sends = experts - local
    halves = HALVES if rows % (HALVES * 16) == 0 else 1
    return [
        pltpu.VMEM((experts, PARTS, depth, cols), jnp.bfloat16),
        pltpu.VMEM((planes, rows, depth), jnp.bfloat16),
        pltpu.VMEM((2, rows), jnp.int32),
        pltpu.VMEM((2, rows), jnp.float32),
        pltpu.VMEM((planes, experts, rows), jnp.float32),
        pltpu.VMEM((planes, rows, experts), jnp.float32),
        pltpu.VMEM((planes * PARTS, rows, cols), jnp.float32),
        pltpu.VMEM((planes + 1, PARTS, rows, cols), jnp.bfloat16),
        dma((local, PARTS)),
        dma((PARTS, sends)),
        dma((experts, PARTS)),
        dma,
        dma((2,)),
        dma((planes,)),
        dma((planes,)),
        dma((planes,)),
        dma((planes,)),
        dma((planes, PARTS, halves)),
        dma((planes + 1, PARTS, halves)),
    ]


def fits(planes, size, tokens, weights):
    local, depth, width = weights.shape
    rows, experts = tokens.shape[0], local * size
    if size & (size - 1) or size < 4 or any(2 * len(group) != BATCH for group in tree(size, local)[0]):
        return False
    held = 2 * experts * depth * width + 2 * planes * rows * depth + 4 * planes * rows * width
    held += 2 * (planes + 2) * rows * width + 4 * planes * rows * (experts + 128)
    return held <= 62 * 2**20


def fused_body(tokens, routes, gates, weights):
    planes, size = lax.axis_size("seq"), lax.axis_size("exp")
    local, depth, width = weights.shape
    rows = tokens.shape[0]
    anywhere = pl.BlockSpec(memory_space=pl.ANY)
    return pl.pallas_call(
        functools.partial(fused_kernel, planes, size),
        out_shape=pltpu.VMEM((rows, width), jnp.bfloat16),
        in_specs=[anywhere] * 4,
        out_specs=pl.BlockSpec(memory_space=pltpu.VMEM),
        scratch_shapes=fused_buffers(planes, size, tokens, weights),
        compiler_params=pltpu.CompilerParams(
            collective_id=0, has_side_effects=True, vmem_limit_bytes=60 * 2**20
        ),
    )(tokens, weights, routes.T, gates.T)


def body(tokens, routes, gates, weights):
    if fits(lax.axis_size("seq"), lax.axis_size("exp"), tokens, weights):
        return fused_body(tokens, routes, gates, weights)
    return spread_body(tokens, routes, gates, weights)


def solution(mesh):
    return jax.shard_map(
        body,
        mesh=mesh,
        in_specs=(
            P(("seq", "exp"), None),
            P(("seq", "exp"), None),
            P(("seq", "exp"), None),
            P("exp", "seq", None),
        ),
        out_specs=P(("seq", "exp"), None),
        check_vma=False,
    )
```

```python
import functools

import jax
import jax.numpy as jnp
from jax import lax
from jax.experimental import pallas as pl
from jax.experimental.pallas import tpu as pltpu
from jax.sharding import PartitionSpec as P

COLUMN_PARTS = (1, 1)


def project_kernel(per_step, x_ref, gate_ref, w_ref, *rest):
    out_ref = rest[-1]
    step = pl.program_id(0)
    lanes = lax.broadcasted_iota(jnp.int32, gate_ref.shape, 1)

    @pl.when(step == 0)
    def _():
        out_ref[...] = jnp.zeros_like(out_ref)

    total = out_ref[...]
    for own in range(per_step):
        expert = step * per_step + own
        gate = jnp.sum(jnp.where(lanes == expert, gate_ref[...], 0.0), axis=1, keepdims=True)
        total += gate * jnp.dot(x_ref[...], w_ref[own], preferred_element_type=jnp.float32)
    out_ref[...] = total


def project(x, gate, weights, before):
    rows, depth = x.shape
    experts, _, cols = weights.shape
    per_step = 2
    return pl.pallas_call(
        functools.partial(project_kernel, per_step),
        grid=(experts // per_step,),
        out_shape=jax.ShapeDtypeStruct((rows, cols), jnp.float32),
        in_specs=[
            pl.BlockSpec((rows, depth), lambda e: (0, 0)),
            pl.BlockSpec((rows, experts), lambda e: (0, 0)),
            pl.BlockSpec((per_step, depth, cols), lambda e: (e, 0, 0)),
        ]
        + [pl.BlockSpec(memory_space=pl.ANY)] * len(before),
        out_specs=pl.BlockSpec((rows, cols), lambda e: (0, 0)),
        compiler_params=pltpu.CompilerParams(vmem_limit_bytes=32 * 1024 * 1024),
        cost_estimate=pl.CostEstimate(
            flops=2 * rows * depth * cols * experts,
            bytes_accessed=2 * experts * depth * cols + 2 * rows * depth,
            transcendentals=0,
        ),
    )(x, gate, weights, *before)


def shift_order(planes):
    near = [d for pair in zip(range(1, planes), range(planes - 1, 0, -1)) for d in pair]
    return list(dict.fromkeys(near))


def unit_order(planes, parts):
    early = 1
    arrival = [0] + shift_order(planes)
    order = [(d, q) for q in range(early) for d in arrival[:-1]]
    order += [(arrival[-1], q) for q in range(early)]
    for q in range(early, parts):
        order += [(d, q) for d in list(range(1, planes)) + [0]]
    return order


def spread_body(tokens, routes, gates, weights):
    experts = weights.shape[0] * lax.axis_size("exp")
    planes = lax.axis_size("seq")
    plane = lax.axis_index("seq")
    depth = weights.shape[1]
    share = weights.shape[2] // sum(COLUMN_PARTS)
    edges = [share * sum(COLUMN_PARTS[:q]) for q in range(len(COLUMN_PARTS) + 1)]

    def moved(value, shift):
        return lax.ppermute(value, "seq", [(i, (i + shift) % planes) for i in range(planes)])

    def features(target):
        return lax.dynamic_slice_in_dim(tokens, target * depth, depth, 1)

    dense = jnp.sum(
        jnp.where(
            routes[:, None, :] == jnp.arange(experts, dtype=jnp.int32)[None, :, None],
            gates[:, None, :],
            0.0,
        ),
        axis=2,
    )
    sent = dense.T
    gate, x = {0: dense}, {0: features(plane)}
    for shift in range(1, planes):
        gate[shift] = moved(sent, shift).T
    latest = None
    for shift in shift_order(planes):
        piece = features(lax.rem(plane + shift, planes))
        if latest is not None:
            piece, _ = lax.optimization_barrier((piece, latest))
        latest = x[shift] = moved(piece, shift)
    whole = [
        lax.all_gather(weights[:, :, edges[q] : edges[q + 1]], "exp", axis=0, tiled=True)
        for q in range(len(COLUMN_PARTS))
    ]
    parts, running, flying, stage, started = {}, {}, {}, {}, {}
    previous = []
    for index, (shift, q) in enumerate(unit_order(planes, len(COLUMN_PARTS))):
        landed = [key for key in flying if started[key] <= index - 2 and index >= planes]
        done = project(x[shift], gate[shift], whole[q], previous + [flying.pop(key) for key in landed])
        previous = [done]
        parts[shift, q] = done
        at = stage.get(q, 1)
        while at <= planes and (at % planes, q) in parts:
            begin = index
            value = parts[at % planes, q]
            if at > 1:
                value = running[q].astype(jnp.float32) + value
                begin = max(begin, started[at - 1, q] + 1)
            running[q] = value.astype(jnp.bfloat16)
            if at < planes:
                running[q] = moved(running[q], 1)
                flying[at, q] = running[q]
                started[at, q] = begin
            at += 1
        stage[q] = at
    return jnp.concatenate([running[q] for q in range(len(COLUMN_PARTS))], axis=1)


MESH = pl.DeviceIdType.MESH
PARTS = 4
BATCH = 4
HALVES = 2
STEP, SLOT, WAIT, OVER = 3.15, 12.0, 2.0, 1.5
HOP_EARLY, HOP, ACROSS, FINAL, MIDDLE = 16.0, 10.0, 15.0, 25.0, 112.0
LANDED = {True: (0.0, 32.0, 62.0, 124.0), False: (0.0, 32.0, 32.0, 97.0)}


def tree(size, local):
    digits = size.bit_length() - 1
    high = list(range(1, digits))

    def order(own):
        turn = own % max(1, len(high))
        return high[turn:] + high[:turn] + [0]

    def last(delta, own):
        return max((order(own).index(b) for b in range(digits) if delta >> b & 1), default=-1)

    def children(delta, own):
        return [b for b in order(own)[last(delta, own) + 1 :]]

    groups = [[(0, own) for own in range(local)]]
    for turn in range(local):
        groups.append([(1 << b, sorted(range(local), key=lambda own: order(own).index(b))[turn]) for b in high])
    for hops in range(2, digits):
        far = [h << 1 for h in range(size // 2) if bin(h).count("1") == hops]
        groups.append([(h, own) for h in far for own in range(local)])
    return groups, children


def line_order(planes):
    middle = (planes - 1) / 2

    def key(p, d):
        hops = abs(d - p)
        return (min(hops, 2), -hops if p in (0, planes - 1) else hops, abs(d - middle), d)

    return [sorted(range(planes), key=functools.partial(key, p)) for p in range(planes)]


def schedule(planes, parts, groups):
    ends = [p in (0, planes - 1) for p in range(planes)]

    def arrival(o, end):
        return LANDED[end][min(o, len(LANDED[end]) - 1)]

    def due(q, g):
        return SLOT * (q * (groups - 1) + g) + WAIT

    def extra(end):
        kind = line_order(planes)[0 if end else 1 % planes]
        tasks = [
            (q, -abs(kind[o] - kind[0]), g, o)
            for q in range(parts)
            for o in range(2, planes)
            for g in range(0, groups, 2)
        ]
        tasks, clock, taken = sorted(tasks), 0.0, {}
        for q in range(parts):
            for g in range(groups):
                clock = max(clock, due(q, g)) + (STEP if q or g % 2 else 0.0)
                if q == 0 and g == groups - 1 and planes > 1:
                    clock = max(clock, arrival(1, end)) + groups // 2 * STEP
                taken[q, g] = []
                follow = due(q, g + 1) if g + 1 < groups else due(q + 1, 0)
                while (q, g) != (parts - 1, groups - 1) and clock + STEP <= follow + OVER:
                    ready = [t for t in tasks if (t[0], t[2] + 1) <= (q, g) and arrival(t[3], end) <= clock]
                    if not ready:
                        break
                    tasks.remove(ready[0])
                    taken[q, g].append((ready[0][3], ready[0][0], ready[0][2]))
                    clock += STEP
        taken["rest"] = [(t[3], t[0], t[2]) for t in tasks]
        return taken

    both = {end: extra(end) for end in (True, False)}
    steps, places = {True: [], False: []}, {}

    def add(work):
        most = max(len(work[end]) for end in work)
        for end in work:
            steps[end] += work[end] + [None] * (most - len(work[end]))

    def halves(work):
        return [((o, q, g), (o, q, g + 1)) for o, q, g in work]

    for q in range(parts):
        for g in range(groups):
            places[q, g] = len(steps[True])
            own = []
            if q == 0:
                if g % 2:
                    own.append(((0, 0, g - 1), (0, 0, g)))
                if g == groups - 1 and planes > 1:
                    own += halves([(1, 0, i) for i in range(0, groups, 2)])
            elif (q, g) != (parts - 1, groups - 1):
                own.append(((0, q, g), (min(1, planes - 1), q, g)))
            add({end: own + halves(both[end][q, g]) for end in both})
    add({end: halves(both[end]["rest"]) for end in both})
    last = ((0, parts - 1, groups - 1), (min(1, planes - 1), parts - 1, groups - 1))
    add({end: [last] for end in both})

    at = {}
    for (q, g), index in places.items():
        at[index] = max(at.get(index, 0.0), due(q, g))
    start, begun, ended = {}, {}, {}
    for end in both:
        clock, start[end] = 0.0, []
        for index, pair in enumerate(steps[end]):
            clock = max([clock, at.get(index, 0.0)] + [arrival(o, end) for o, _, _ in pair or []])
            start[end].append(clock)
            clock += STEP if pair else 0.0
            for o, q, _ in pair or []:
                begun.setdefault((end, o), index)
                ended[end, o, q] = clock
    order = line_order(planes)
    ready = {}
    for q in range(parts):
        for d in range(planes):
            for p in list(range(d)) + list(range(planes - 1, d, -1)) + [d]:
                time = ended[ends[p], order[p].index(d), q]
                before = [p - 1] if p < d else [p + 1] if p > d else [p - 1, p + 1]
                for other in before:
                    if 0 <= other < planes:
                        sent = ready[other, d, q]
                        hop = HOP_EARLY if sent < LANDED[False][-1] else HOP
                        time = max(time, sent + (hop if ends[p] or ends[other] else ACROSS))
                onward = p + 1 if p < d else p - 1
                if p != d and not ends[p] and not ends[onward]:
                    time = max(time, MIDDLE)
                ready[p, d, q] = time + (FINAL if p == d else 0.0)
    sums = {}
    for p in range(planes):
        end = len(steps[True])
        for time, d, q in sorted((ready[p, d, q], d, q) for d in range(planes) for q in range(parts)):
            where = next((i for i, begin in enumerate(start[ends[p]]) if begin >= time), None)
            if where is None:
                where, end = end, end + 1
            sums.setdefault(where, {}).setdefault(p, []).append((d, q))
    events = {}
    for key, index in places.items():
        events.setdefault(index, []).append(key)
    return steps, events, begun, sums


def pick(which, values, default=0):
    found = jnp.int32(default)
    for index, value in enumerate(values):
        found = jnp.where(which == index, jnp.int32(value), found)
    return found


def fused_kernel(planes, size, tokens, weights, routes, gates, out, *scratch):
    w_buf, x_buf, r_buf, v_buf, t_buf, g_buf, acc, s_buf = scratch[:8]
    w_load, w_send, w_recv, x_load, r_load, x_send, x_recv, t_send, t_recv, s_send, s_recv = scratch[8:]
    plane, me = lax.axis_index("seq"), lax.axis_index("exp")
    local = weights.shape[0]
    rows, depth = x_buf.shape[1:]
    parts, cols = w_buf.shape[1], w_buf.shape[3]
    halves = s_recv.shape[2]
    batches = w_buf.shape[0] // BATCH
    groups, children = tree(size, local)
    arrival = [chunk for group in groups for chunk in group + [(delta | 1, own) for delta, own in group]]
    place = {chunk: index for index, chunk in enumerate(arrival)}
    digits = size.bit_length() - 1
    steps, events, begun, sums = schedule(planes, parts, len(groups))
    orders = line_order(planes)
    at_end = (plane == 0) | (plane == planes - 1)
    planes_of = [pick(plane, [orders[p][o] for p in range(planes)]) for o in range(planes)]
    near = [me + (1 - 2 * (lax.div(me, jnp.int32(1 << b)) % 2)) * (1 << b) for b in range(digits)]

    barrier = pltpu.get_barrier_semaphore()
    own_loads = [
        pltpu.make_async_copy(
            weights.at[own, :, pl.ds(q * cols, cols)], w_buf.at[place[0, own], q], w_load.at[own, q]
        )
        for q in range(parts)
        for own in range(local)
    ]
    own_rows = pltpu.make_async_copy(
        tokens.at[:, pl.ds(pl.multiple_of(plane * depth, depth), depth)], x_buf.at[plane], x_load
    )
    small = [pltpu.make_async_copy(routes, r_buf, r_load.at[0]), pltpu.make_async_copy(gates, v_buf, r_load.at[1])]
    for load in own_loads[:local] + small:
        load.start()
    for b in range(digits):
        pl.semaphore_signal(barrier, inc=1, device_id={"exp": near[b]}, device_id_type=MESH)
    for shift in range(1, planes):
        pl.semaphore_signal(
            barrier, inc=1, device_id={"seq": lax.rem(plane + shift, planes)}, device_id_type=MESH
        )
    pl.semaphore_wait(barrier, digits + planes - 1)

    def rows_to(target):
        return pltpu.make_async_remote_copy(
            src_ref=tokens.at[:, pl.ds(pl.multiple_of(target * depth, depth), depth)],
            dst_ref=x_buf.at[plane],
            send_sem=x_send.at[target],
            recv_sem=x_recv.at[plane],
            device_id={"seq": target},
            device_id_type=MESH,
        )

    def gates_to(target):
        return pltpu.make_async_remote_copy(
            src_ref=t_buf.at[plane],
            dst_ref=t_buf.at[plane],
            send_sem=t_send.at[target],
            recv_sem=t_recv.at[plane],
            device_id={"seq": target},
            device_id_type=MESH,
        )

    def spread(distance, outer):
        for target in (plane + distance, plane - distance):
            end = (target == 0) | (target == planes - 1)

            @pl.when((target >= 0) & (target < planes) & (end if outer else jnp.logical_not(end)))
            def _():
                rows_to(target).start()

    far = [(distance, outer) for distance in range(3, planes) for outer in (True, False)]
    leave = {
        (0, 0): [(1, True), (1, False)],
        (0, len(groups) - 1): far,
        (parts - 3, 2): [(2, False)],
        (parts - 2, 1): [(2, True)],
    }
    sent = []

    def pass_on(delta, own, b, q):
        copy = pltpu.make_async_remote_copy(
            src_ref=w_buf.at[place[delta, own], q],
            dst_ref=w_buf.at[place[delta ^ (1 << b), own], q],
            send_sem=w_send.at[q, count(delta, own, b)],
            recv_sem=w_recv.at[place[delta ^ (1 << b), own], q],
            device_id={"exp": near[b]},
            device_id_type=MESH,
        )
        return copy

    edges = [(delta, own, b) for group in groups for delta, own in group for b in children(delta, own)]

    def count(*edge):
        return edges.index(edge)

    def send_own(q):
        for own in range(local):
            own_loads[q * local + own].wait()
        for group in groups[1 : local + 1]:
            for delta, own in group:
                pass_on(0, own, delta.bit_length() - 1, q).start()
        for own in range(local):
            pass_on(0, own, 0, q).start()

    def landing(chunk, q):
        index = place[chunk]
        return pltpu.make_async_copy(w_buf.at[index, q], w_buf.at[index, q], w_recv.at[index, q])

    def arrive(q, g):
        for distance, outer in leave.get((q, g), []):
            if distance < planes:
                spread(distance, outer)
        if g == 0 and q == 0:
            send_own(0)
            own_rows.start()
            for load in own_loads[local:]:
                load.start()
            clear()
            own_gates()
        if g > 0:
            for delta, own in groups[g]:
                landing((delta, own), q).wait()
                for b in children(delta, own):
                    pass_on(delta, own, b, q).start()
        if (q, g) == (0, 1):
            for turn in range(1, planes):
                gates_to(planes_of[turn]).start()
        if g == len(groups) - 2 and q + 1 < parts:
            send_own(q + 1)
        for delta, own in groups[g]:
            landing((delta | 1, own), q).wait()

    def own_gates():
        for load in small:
            load.wait()
        row = lax.broadcasted_iota(jnp.int32, t_buf.shape[1:], 0)
        expert = jnp.zeros(t_buf.shape[1:], jnp.int32)
        for index, (delta, own) in enumerate(arrival):
            source = me + sum(near[b] - me for b in range(digits) if delta >> b & 1)
            expert = jnp.where(row == index, source * local + own, expert)
        t_buf[plane] = sum(
            jnp.where(r_buf[k : k + 1, :] == expert, v_buf[k : k + 1, :], 0.0) for k in range(r_buf.shape[0])
        )

    def clear():
        acc[...] = jnp.zeros_like(acc)

        @pl.when(plane == 0)
        def _():
            for slot in range(planes):
                s_buf[slot] = jnp.zeros(s_buf.shape[1:], s_buf.dtype)

        @pl.when(plane == planes - 1)
        def _():
            for slot in [*range(planes - 1), planes]:
                s_buf[slot] = jnp.zeros(s_buf.shape[1:], s_buf.dtype)

    def meet(o):
        d = planes_of[o]
        if o == 0:
            own_rows.wait()
            g_buf[d] = t_buf[d].T
        else:
            pltpu.make_async_copy(x_buf.at[d], x_buf.at[d], x_recv.at[d]).wait()
            pltpu.make_async_copy(t_buf.at[d], t_buf.at[d], t_recv.at[d]).wait()
            g_buf[d] = t_buf[d].T

    span = rows // halves
    block = span

    def sum_out(d, o, q, half):
        right = d > plane
        onward = jnp.where(right, plane + 1, plane - 1)
        slot = jnp.where(jnp.logical_not(right) & (onward == d), planes, d)
        part = pl.ds(half * span, span)
        return pltpu.make_async_remote_copy(
            src_ref=s_buf.at[d, q, part],
            dst_ref=s_buf.at[slot, q, part],
            send_sem=s_send.at[o, q, half],
            recv_sem=s_recv.at[slot, q, half],
            device_id={"seq": onward},
            device_id_type=MESH,
        )

    def summed(slot, q, half):
        part = s_buf.at[slot, q, pl.ds(half * span, span)]
        return pltpu.make_async_copy(part, part, s_recv.at[slot, q, half])

    def final(q):
        for half in range(halves):

            @pl.when(plane > 0)
            def _():
                summed(plane, q, half).wait()

            @pl.when(plane < planes - 1)
            def _():
                summed(planes, q, half).wait()

            @pl.loop(half * span // block, (half + 1) * span // block)
            def _(i):
                part = pl.ds(pl.multiple_of(i * block, block), block)
                sides = s_buf[plane, q, part].astype(jnp.float32) + s_buf[planes, q, part].astype(jnp.float32)
                total = acc[q, part] + sides
                out[part, pl.ds(pl.multiple_of(q * cols, cols), cols)] = total.astype(out.dtype)

    def onward(d, o, q, ahead):
        for half in range(halves):
            if ahead is not None:

                @pl.when(ahead[0] >= 0)
                def _():
                    sum_out(*ahead, half).wait_send()


            @pl.when(jnp.where(d > plane, plane > 0, plane < planes - 1))
            def _():
                summed(d, q, half).wait()

            @pl.loop(half * span // block, (half + 1) * span // block)
            def _(i):
                part = pl.ds(pl.multiple_of(i * block, block), block)
                total = acc[o * parts + q, part] + s_buf[d, q, part].astype(jnp.float32)
                s_buf[d, q, part] = total.astype(s_buf.dtype)

            sum_out(d, o, q, half).start()

    total_steps = len(steps[True])
    waited = {}

    def behind(p, index, d):
        way = [k for k in range(total_steps, index) for e, _ in sums.get(k, {}).get(p, []) if e != p and (e > p) == (d > p)]
        return next(t for t in sums[way[-1]][p]) if way else None

    def settle(index):
        by_plane = sums[index]
        most = max(len(todo) for todo in by_plane.values())
        for turn in range(most):
            todo = [by_plane.get(p, [])[turn : turn + 1] for p in range(planes)]
            d = pick(plane, [t[0][0] if t else -1 for t in todo], -1)
            q = pick(plane, [t[0][1] if t else 0 for t in todo])
            o = pick(plane, [orders[p].index(t[0][0]) if t else 0 for p, t in enumerate(todo)])
            if any(t and t[0][0] == p for p, t in enumerate(todo)):

                @pl.when(d == plane)
                def _():
                    final(q)

            if any(t and t[0][0] != p for p, t in enumerate(todo)):
                ahead = [behind(p, index, t[0][0]) if t and t[0][0] != p else None for p, t in enumerate(todo)]
                before_it = None
                if any(ahead):
                    before_it = (
                        pick(plane, [a[0] if a else -1 for a in ahead], -1),
                        pick(plane, [orders[p].index(a[0]) if a else 0 for p, a in enumerate(ahead)]),
                        pick(plane, [a[1] if a else 0 for a in ahead]),
                    )

                @pl.when((d >= 0) & (d != plane))
                def _():
                    onward(d, o, q, before_it)

    lanes = lax.broadcasted_iota(jnp.int32, (rows, g_buf.shape[2]), 1)
    def before(index, at):
        @pl.when(index == at)
        def _():
            early = at in sums and (parts - 1, len(groups) - 1) in events.get(at, [])
            if early:
                settle(at)
            for key in events.get(at, []):
                arrive(*key)
            for (end, o), index_of in begun.items():
                if index_of == at and begun[not end, o] == at:
                    if end:
                        meet(o)
                elif index_of == at:

                    @pl.when(at_end if end else jnp.logical_not(at_end))
                    def _():
                        meet(o)
            if at in sums and not early:
                settle(at)

    def search(index, points):
        if len(points) == 1:
            before(index, points[0])
        elif points:
            half = len(points) // 2

            @pl.when(index < points[half])
            def _():
                search(index, points[:half])

            @pl.when(index >= points[half])
            def _():
                search(index, points[half:])

    def products(code):
        o, q, g = code // (parts * batches), (code // batches) % parts, code % batches
        d = pick(o, [0])
        for turn in range(planes):
            d = jnp.where(o == turn, planes_of[turn], d)
        total = None
        for turn in range(BATCH):
            expert = g * BATCH + turn
            gate = jnp.sum(jnp.where(lanes == expert, g_buf[d], 0.0), axis=1, keepdims=True)
            term = gate * jnp.dot(x_buf[d], w_buf[expert, q], preferred_element_type=jnp.float32)
            total = term if total is None else total + term
        acc[o * parts + q] += total

    def code_of(pair, side):
        if pair is None:
            return -1
        o, q, g = pair[side]
        return (o * parts + q) * batches + g

    points = sorted({*events, *begun.values(), *(k for k in sums if k < total_steps)})

    @pl.loop(0, total_steps)
    def _(index):
        search(index, points)
        codes = []
        for side in range(2):
            ways = [pick(index, [code_of(pair, side) for pair in steps[end]]) for end in (True, False)]
            codes.append(jnp.where(at_end, *ways))

        @pl.when(codes[0] >= 0)
        def _():
            for code in codes:
                products(code)

    def sent_by(p, early):
        for at in sums:
            for d, q in sums[at].get(p, []):
                if d != p and (at < total_steps) == early:
                    yield orders[p].index(d), q

    def drain(early):
        for o in range(1, planes):
            for q in range(parts):
                senders = [p for p in range(planes) if (o, q) in sent_by(p, early) and p not in waited.get((o, q), [])]
                if senders:

                    @pl.when(functools.reduce(jnp.logical_or, [plane == p for p in senders]))
                    def _():
                        for half in range(halves):
                            sum_out(planes_of[o], o, q, half).wait_send()

    tail = sorted(k for k in sums if k >= total_steps)
    for at in tail:
        for p in sums[at]:
            for d, _ in sums[at][p]:
                a = behind(p, at, d) if d != p else None
                if a:
                    waited.setdefault((orders[p].index(a[0]), a[1]), []).append(p)
    for at in tail:
        settle(at)
        if at == tail[0]:
            drain(True)
            for q in range(parts):
                for edge in edges:
                    pass_on(*edge, q).wait_send()
            for o in range(1, planes):
                rows_to(planes_of[o]).wait_send()
                gates_to(planes_of[o]).wait_send()
    drain(False)


def fused_buffers(planes, size, tokens, weights):
    local, depth, width = weights.shape
    rows, cols, experts = tokens.shape[0], width // PARTS, local * size
    dma = pltpu.SemaphoreType.DMA
    sends = experts - local
    halves = HALVES if rows % (HALVES * 16) == 0 else 1
    return [
        pltpu.VMEM((experts, PARTS, depth, cols), jnp.bfloat16),
        pltpu.VMEM((planes, rows, depth), jnp.bfloat16),
        pltpu.VMEM((2, rows), jnp.int32),
        pltpu.VMEM((2, rows), jnp.float32),
        pltpu.VMEM((planes, experts, rows), jnp.float32),
        pltpu.VMEM((planes, rows, experts), jnp.float32),
        pltpu.VMEM((planes * PARTS, rows, cols), jnp.float32),
        pltpu.VMEM((planes + 1, PARTS, rows, cols), jnp.bfloat16),
        dma((local, PARTS)),
        dma((PARTS, sends)),
        dma((experts, PARTS)),
        dma,
        dma((2,)),
        dma((planes,)),
        dma((planes,)),
        dma((planes,)),
        dma((planes,)),
        dma((planes, PARTS, halves)),
        dma((planes + 1, PARTS, halves)),
    ]


def fits(planes, size, tokens, weights):
    local, depth, width = weights.shape
    rows, experts = tokens.shape[0], local * size
    if size & (size - 1) or size < 4 or any(2 * len(group) != BATCH for group in tree(size, local)[0]):
        return False
    held = 2 * experts * depth * width + 2 * planes * rows * depth + 4 * planes * rows * width
    held += 2 * (planes + 2) * rows * width + 4 * planes * rows * (experts + 128)
    return held <= 62 * 2**20


def fused_body(tokens, routes, gates, weights):
    planes, size = lax.axis_size("seq"), lax.axis_size("exp")
    local, depth, width = weights.shape
    rows = tokens.shape[0]
    anywhere = pl.BlockSpec(memory_space=pl.ANY)
    return pl.pallas_call(
        functools.partial(fused_kernel, planes, size),
        out_shape=pltpu.VMEM((rows, width), jnp.bfloat16),
        in_specs=[anywhere] * 4,
        out_specs=pl.BlockSpec(memory_space=pltpu.VMEM),
        scratch_shapes=fused_buffers(planes, size, tokens, weights),
        compiler_params=pltpu.CompilerParams(
            collective_id=0, has_side_effects=True, vmem_limit_bytes=60 * 2**20
        ),
    )(tokens, weights, routes.T, gates.T)


def body(tokens, routes, gates, weights):
    if fits(lax.axis_size("seq"), lax.axis_size("exp"), tokens, weights):
        return fused_body(tokens, routes, gates, weights)
    return spread_body(tokens, routes, gates, weights)


def solution(mesh):
    return jax.shard_map(
        body,
        mesh=mesh,
        in_specs=(
            P(("seq", "exp"), None),
            P(("seq", "exp"), None),
            P(("seq", "exp"), None),
            P("exp", "seq", None),
        ),
        out_specs=P(("seq", "exp"), None),
        check_vma=False,
    )
```
